256 devices in a mesh: dx: 8 (over x, z_hi), dy: 32 (over y, z_lo, core).
Axes of the slice: x: 4, y: 4, z: 8 (z_hi: 2, z_lo: 4; z = z_hi * 4 + z_lo), core: 2. Of those that a mesh axis runs over, the one named last changes fastest.
Arguments:
- seg_mid: float32 [8, 32, 3, 4096], P('dx', 'dy'), may hold values from 0 to 1
- seg_line: float32 [8, 32, 3, 4096], P('dx', 'dy'), may hold values from -0.3 to 0.3
- seg_burgers: float32 [8, 32, 3, 4096], P('dx', 'dy'), may hold values from -5 to 5
- seg_cell: int32 [8, 32, 4096], P('dx', 'dy'), may hold values from 0 to 71, as said below
- seg_node: int32 [8, 32, 2, 4096], P('dx', 'dy'), may hold values from 0 to 4607, as said below
- ghost_list: int32 [8, 32, 8, 2], P('dx', 'dy'), may hold values from 0 to 31
- ghost_count: int32 [8, 32, 8], P('dx', 'dy'), may hold values from 1 to 2
- pair_list: int32 [8, 32, 32, 12], P('dx', 'dy'), may hold values from 0 to 47, as said below
- pair_count: int32 [8, 32, 32], P('dx', 'dy'), may hold values from 1 to 12
Outputs:
- node_force: float32 [8, 32, 3, 512], P('dx', 'dy')
- cell_moments: float32 [315, 2048], P(None, ('dx', 'dy'))
The draws below stay inside these ranges and needn't reach their ends.
Inputs may be any that keep to these rules, and one draw needn't show every extreme that they name: `seg_node`: each entry is d * 512 + m with m a node of the domain at offset (a, b) from the segment's domain, d = 3 (a + 1) + (b + 1), a and b in -1, 0, 1; d = 4 is the domain itself. `seg_cell`: each entry is d * 8 + c with c a cell owned by the domain at offset (a, b) from the segment's domain, d = 3 (a + 1) + (b + 1), a and b in -1, 0, 1; d = 4 is the domain itself. `pair_list`: the entries of one tile's list are distinct.
All inputs are finite; a program needn't handle non-finite values.
Results may differ from the reference program's by a relative error of at most 0.0003.
Values sent between devices are 32-bit elements; how exact they have to be, the bound alone decides.
A program may use at most 64 MiB of HBM per device.

```python
import jax
import jax.numpy as jnp
import numpy as np
from jax import lax

TILE = 128
TILES = 32
GHOST = 2
NP = 12
NODE_DEV = 512
CELL_DEV = 8
COMPONENTS = 315
SEG_DEV = 4096
POOL = 48
CELLS = 2048
N_DX = 8
N_DY = 32


def draw_seg_node(key, part):
    stay_key, other_key, local_key = jax.random.split(jax.random.fold_in(key, 11), 3)
    shape = (N_DX, N_DY, 2, TILES * TILE)
    staying = jax.random.randint(stay_key, shape, 0, 2)
    elsewhere = jax.random.randint(other_key, shape, 0, 8)
    elsewhere = elsewhere + (elsewhere >= 4).astype(jnp.int32)
    direction = jnp.where(staying == 1, 4, elsewhere)
    local_node = jax.random.randint(local_key, shape, 0, NODE_DEV)
    return (direction * NODE_DEV + local_node).astype(jnp.int32)


def draw_seg_cell(key, part):
    stay_key, other_key, local_key = jax.random.split(jax.random.fold_in(key, 37), 3)
    shape = (N_DX, N_DY, TILES * TILE)
    staying = jax.random.randint(stay_key, shape, 0, 2)
    elsewhere = jax.random.randint(other_key, shape, 0, 8)
    elsewhere = elsewhere + (elsewhere >= 4).astype(jnp.int32)
    direction = jnp.where(staying == 1, 4, elsewhere)
    local_cell = jax.random.randint(local_key, shape, 0, CELL_DEV)
    return (direction * CELL_DEV + local_cell).astype(jnp.int32)


def draw_pair_list(key, part):
    pool_size = TILES + 8 * GHOST
    scores = jax.random.randint(jax.random.fold_in(key, 23), (N_DX, N_DY, TILES, pool_size), 0, 1 << 20)
    scores = scores * pool_size + jnp.arange(pool_size, dtype=jnp.int32)
    ranking = jnp.argsort(scores, axis=-1)
    return ranking[..., :NP].astype(jnp.int32)


def touch_ends(result, rng, smallest, top_value):
    shape = result.shape
    index_at = [jax.random.randint(jax.random.fold_in(rng, axis), (), 0, shape[axis]) for axis in range(len(shape))]
    result = result.at[tuple(index_at)].set(smallest)
    longest = shape.index(max(shape))
    index_at[longest] = (index_at[longest] + 1) % shape[longest]
    return result.at[tuple(index_at)].set(top_value)


def block_scale(key, dims, cuts, least, largest):
    factor_of, own = 1.0, jax.random.fold_in(key, 6)
    for dim, blocks in cuts:
        steps = jnp.exp(jax.random.uniform(jax.random.fold_in(own, dim), (blocks,), jnp.float32, least / len(cuts), largest / len(cuts)))
        factor_of = factor_of * jnp.repeat(steps, dims[dim] // blocks).reshape([-1 if axis == dim else 1 for axis in range(len(dims))])
    return factor_of


def normal_values(key, extent, width, bound, pieces=(), kind=jnp.bfloat16):
    values = width * jax.random.normal(key, extent, jnp.float32)
    if pieces:
        values = values * block_scale(key, extent, pieces, -0.22, 0.18)
    return jnp.clip(values, -bound, bound).astype(kind)


def setup_inputs(seed: int = 0) -> dict:
    streams_of = jax.random.split(jax.random.key(seed), 10)
    seg_mid = jnp.clip(1.0 * jax.random.uniform(streams_of[0], (N_DX, N_DY, 3, SEG_DEV), jnp.float32) ** block_scale(streams_of[0], (N_DX, N_DY, 3, SEG_DEV), ((0, 8), (1, 32)), -0.2, 0.2), 0.0, 1.0)
    seg_line = normal_values(streams_of[1], (N_DX, N_DY, 3, SEG_DEV), 0.05, 0.3, ((0, 8), (1, 32)), jnp.float32)
    seg_burgers = normal_values(streams_of[2], (N_DX, N_DY, 3, SEG_DEV), 1.0, 5.0, ((0, 8), (1, 32)), jnp.float32)
    seg_cell = draw_seg_cell(jax.random.fold_in(streams_of[9], 71), 0)
    seg_node = draw_seg_node(jax.random.fold_in(streams_of[9], 71), 0)
    ghost_list = touch_ends(jax.random.randint(streams_of[5], (N_DX, N_DY, 8, GHOST), 0, TILES), jax.random.fold_in(streams_of[5], 1), 0, TILES - 1).astype(jnp.int32)
    ghost_count = touch_ends(jax.random.randint(streams_of[6], (N_DX, N_DY, 8), 1, GHOST + 1), jax.random.fold_in(streams_of[6], 1), 1, GHOST).astype(jnp.int32)
    pair_list = draw_pair_list(jax.random.fold_in(streams_of[9], 71), 0)
    pair_count = touch_ends(jax.random.randint(streams_of[8], (N_DX, N_DY, TILES), 1, NP + 1), jax.random.fold_in(streams_of[8], 1), 1, NP).astype(jnp.int32)
    return dict(seg_mid=seg_mid, seg_line=seg_line, seg_burgers=seg_burgers, seg_cell=seg_cell, seg_node=seg_node, ghost_list=ghost_list, ghost_count=ghost_count, pair_list=pair_list, pair_count=pair_count)


core_radius = 0.1
shear_scale = 0.25
neighbour_offsets = ((-1, -1), (-1, 0), (-1, 1), (0, -1), (0, 1), (1, -1), (1, 0), (1, 1))

def exponent_table():
    exponent_rows = []
    for degree in range(5):
        for first_power in range(degree, -1, -1):
            for second in range(degree - first_power, -1, -1):
                exponent_rows.append((first_power, second, degree - first_power - second))
    return np.array(exponent_rows, dtype=np.int32)

def moment_terms(midpoint, line_vector, burgers):
    scaled = 2.0 * (midpoint - 0.5)
    powers = jnp.stack([jnp.ones_like(scaled), scaled, scaled * scaled, scaled ** 3, scaled ** 4], axis=1)
    exponents = exponent_table()
    monomial = powers[0, exponents[:, 0]] * powers[1, exponents[:, 1]] * powers[2, exponents[:, 2]]
    products = (burgers[:, None, :] * line_vector[None, :, :]).reshape(9, -1)
    return (products[:, None, :] * monomial[None, :, :]).reshape(9 * monomial.shape[0], -1)

def pair_stress(field_tiles, source_tiles, valid_weight):
    separation = [field_tiles[component][:, :, None] - source_tiles[component][:, None, :] for component in range(3)]
    line_source = source_tiles[3:6]
    burgers_source = source_tiles[6:9]
    cross_source = [burgers_source[1] * line_source[2] - burgers_source[2] * line_source[1], burgers_source[2] * line_source[0] - burgers_source[0] * line_source[2], burgers_source[0] * line_source[1] - burgers_source[1] * line_source[0]]
    cross_source = [entry_value[:, None, :] for entry_value in cross_source]
    radius_sq = separation[0] ** 2 + separation[1] ** 2 + separation[2] ** 2 + core_radius ** 2
    inverse = 1.0 / jnp.sqrt(radius_sq)
    weight = shear_scale * valid_weight[:, None, None] * inverse / radius_sq
    projection = separation[0] * cross_source[0] + separation[1] * cross_source[1] + separation[2] * cross_source[2]
    diagonal_term = projection * (1.0 + 1.5 * core_radius ** 2 / radius_sq)
    entries = []
    for first_axis, second_axis in ((0, 0), (1, 1), (2, 2), (0, 1), (0, 2), (1, 2)):
        entry_value = separation[first_axis] * cross_source[second_axis] + separation[second_axis] * cross_source[first_axis] - 3.0 * projection * separation[first_axis] * separation[second_axis] / radius_sq
        if first_axis == second_axis:
            entry_value = entry_value + diagonal_term
        entries.append(lax.optimization_barrier(jnp.sum(weight * entry_value, axis=2)))
    return jnp.stack(entries)

def segment_force(stress, own_columns):
    line_vector = own_columns[3:6]
    burgers = own_columns[6:9]
    traction = [stress[0] * burgers[0] + stress[3] * burgers[1] + stress[4] * burgers[2], stress[3] * burgers[0] + stress[1] * burgers[1] + stress[5] * burgers[2], stress[4] * burgers[0] + stress[5] * burgers[1] + stress[2] * burgers[2]]
    return jnp.stack([traction[1] * line_vector[2] - traction[2] * line_vector[1], traction[2] * line_vector[0] - traction[0] * line_vector[2], traction[0] * line_vector[1] - traction[1] * line_vector[0]])

def reference(seg_mid, seg_line, seg_burgers, seg_cell, seg_node, ghost_list, ghost_count, pair_list, pair_count):
    width_x = seg_mid.shape[0]
    width_y = seg_mid.shape[1]
    seg_data = jnp.concatenate([seg_mid, seg_line, seg_burgers], axis=2)
    own_tiles = seg_data.reshape(width_x, width_y, 9, TILES, TILE).transpose(0, 1, 3, 2, 4)
    packets = jax.vmap(jax.vmap(lambda tile_set, chosen: tile_set[chosen]))(own_tiles, ghost_list)
    slot_valid = (jnp.arange(GHOST, dtype=jnp.int32)[None, None, None, :] < ghost_count[..., None]).astype(jnp.float32)
    packets = packets * slot_valid[..., None, None]
    groups = []
    for group_index in range(8):
        first_shift, second_shift = neighbour_offsets[group_index]
        incoming = jnp.roll(packets[:, :, 7 - group_index], shift=(-first_shift, -second_shift), axis=(0, 1))
        offset_rows = jnp.array([first_shift, second_shift, 0, 0, 0, 0, 0, 0, 0], jnp.float32)
        groups.append(incoming + offset_rows[None, None, None, :, None])
    source_pool = jnp.concatenate([own_tiles] + groups, axis=2)
    total_domains = width_x * width_y

    def domain_partial(inputs):
        pool_dev, own_dev, pairs_dev, limit_dev, ends_dev = inputs
        own_columns = own_dev.transpose(1, 0, 2)

        def add_slot(stress_total, slot_index):
            source_tiles = pool_dev[pairs_dev[:, slot_index]].transpose(1, 0, 2)
            valid_weight = (slot_index < limit_dev).astype(jnp.float32)
            return (stress_total + pair_stress(own_columns, source_tiles, valid_weight), None)
        stress_total, unused = lax.scan(add_slot, jnp.zeros((6, TILES, TILE), jnp.float32), jnp.arange(NP, dtype=jnp.int32))
        force = segment_force(stress_total, own_columns).reshape(3, TILES * TILE)
        halves = 0.5 * force.T
        partial_value = jax.ops.segment_sum(jnp.concatenate([halves, halves], axis=0), jnp.concatenate([ends_dev[0], ends_dev[1]]).astype(jnp.int32), num_segments=9 * NODE_DEV)
        return partial_value.reshape(9, NODE_DEV, 3).transpose(0, 2, 1)
    partials = lax.map(domain_partial, (source_pool.reshape(total_domains, POOL, 9, TILE), own_tiles.reshape(total_domains, TILES, 9, TILE), pair_list.reshape(total_domains, TILES, NP), pair_count.reshape(total_domains, TILES), seg_node.reshape(total_domains, 2, TILES * TILE)))
    partials = partials.reshape(width_x, width_y, 9, 3, NODE_DEV)
    node_force = jnp.zeros((width_x, width_y, 3, NODE_DEV), jnp.float32)
    for direction in range(9):
        node_force = node_force + jnp.roll(partials[:, :, direction], shift=(direction // 3 - 1, direction % 3 - 1), axis=(0, 1))

    def cell_partial(inputs):
        mid_dev, line_dev, burgers_dev, cell_dev = inputs
        terms = moment_terms(mid_dev, line_dev, burgers_dev)
        return jax.ops.segment_sum(terms.T, cell_dev.astype(jnp.int32), num_segments=9 * CELL_DEV)
    cell_parts = lax.map(cell_partial, (seg_mid.reshape(total_domains, 3, TILES * TILE), seg_line.reshape(total_domains, 3, TILES * TILE), seg_burgers.reshape(total_domains, 3, TILES * TILE), seg_cell.reshape(total_domains, TILES * TILE)))
    cell_parts = cell_parts.reshape(width_x, width_y, 9, CELL_DEV, COMPONENTS)
    cell_grid = jnp.zeros((width_x, width_y, CELL_DEV, COMPONENTS), jnp.float32)
    for direction in range(9):
        cell_grid = cell_grid + jnp.roll(cell_parts[:, :, direction], shift=(direction // 3 - 1, direction % 3 - 1), axis=(0, 1))
    return (node_force, cell_grid.reshape(CELLS, COMPONENTS).T)
```

```python
import jax
import jax.numpy as jnp
from jax import lax
from jax.experimental import pallas as pl
from jax.experimental.pallas import tpu as pltpu
from jax.sharding import PartitionSpec as P

TILE = 128
TILES = 32
GHOST = 2
NP = 12
NODE_DEV = 512
CELL_DEV = 8
COMPONENTS = 315
POOL = 48
FEATURES = 40
AUG = 32
TERMS = 368

core_radius = 0.1
shear_scale = 0.25
neighbour_offsets = ((-1, -1), (-1, 0), (-1, 1), (0, -1), (0, 1), (1, -1), (1, 0), (1, 1))
f32 = jnp.float32
bf16 = jnp.bfloat16
MESH = pl.DeviceIdType.MESH
NT = (((1,), (1,)), ((), ()))


def rounded(value):
    return value.astype(bf16).astype(f32)


def pieces(value, count):
    parts = []
    for _ in range(count - 1):
        part = rounded(value)
        parts.append(part)
        value = value - part
    parts.append(rounded(value))
    return parts


def exponent_table():
    exponent_rows = []
    for degree in range(5):
        for first_power in range(degree, -1, -1):
            for second in range(degree - first_power, -1, -1):
                exponent_rows.append((first_power, second, degree - first_power - second))
    return exponent_rows


def cross(u, v):
    return [
        u[1] * v[2] - u[2] * v[1],
        u[2] * v[0] - u[0] * v[2],
        u[0] * v[1] - u[1] * v[0],
    ]


def dot3(u, v):
    return u[0] * v[0] + u[1] * v[1] + u[2] * v[2]


PAIRS6 = ((0, 0), (1, 1), (2, 2), (0, 1), (0, 2), (1, 2))
SYM = {}
for _slot, (_m, _n) in enumerate(PAIRS6):
    SYM[(_m, _n)] = _slot
    SYM[(_n, _m)] = _slot


def source_features(y, line, burgers):
    g = [shear_scale * v for v in cross(burgers, line)]
    h = [[y[k] * g[n] for n in range(3)] for k in range(3)]
    q = [[y[k] * h[l][n] for n in range(3)] for (k, l) in PAIRS6]
    y2 = dot3(y, y)
    trace = h[0][0] + h[1][1] + h[2][2]
    c = []
    for m, n in PAIRS6:
        value = y2 * (h[m][n] + h[n][m]) - 3.0 * trace * (y[m] * y[n])
        if m == n:
            value = value + y2 * trace
        c.append(value)
    rows = list(g)
    for k in range(3):
        rows += h[k]
    for kl in range(6):
        rows += q[kl]
    rows += c
    return rows


def stress_from_moments(x, moment):
    c2 = core_radius**2
    G = moment[0:3]
    H = [moment[3 + 3 * k : 6 + 3 * k] for k in range(3)]
    Q = [moment[12 + 3 * kl : 15 + 3 * kl] for kl in range(6)]
    C = moment[30:36]
    x2 = dot3(x, x)
    xG = dot3(x, G)
    trH = H[0][0] + H[1][1] + H[2][2]
    Z = [Q[0][n] + Q[1][n] + Q[2][n] for n in range(3)]
    W = [Q[SYM[(0, n)]][0] + Q[SYM[(1, n)]][1] + Q[SYM[(2, n)]][2] for n in range(3)]
    xH = [x[0] * H[0][n] + x[1] * H[1][n] + x[2] * H[2][n] for n in range(3)]
    Hx = [H[n][0] * x[0] + H[n][1] * x[1] + H[n][2] * x[2] for n in range(3)]
    xQ = [
        [x[0] * Q[SYM[(0, m)]][n] + x[1] * Q[SYM[(1, m)]][n] + x[2] * Q[SYM[(2, m)]][n] for n in range(3)]
        for m in range(3)
    ]
    lead = [(x2 + c2) * G[n] - 2.0 * xH[n] + Z[n] + 3.0 * Hx[n] - 3.0 * W[n] for n in range(3)]
    both = xG - trH
    diagonal = (
        (x2 + 2.5 * c2) * both
        - 2.0 * dot3(x, xH)
        + 2.0 * dot3(x, W)
        + dot3(x, Z)
    )
    out = []
    for m, n in PAIRS6:
        value = (
            x[m] * lead[n]
            + x[n] * lead[m]
            - (x2 + c2) * (H[m][n] + H[n][m])
            + 2.0 * (xQ[m][n] + xQ[n][m])
            - 3.0 * (x[m] * x[n] * both + dot3(x, Q[SYM[(m, n)]]))
            - C[SYM[(m, n)]]
        )
        if m == n:
            value = value + diagonal
        out.append(value)
    return out


PIECE_X = (0, 0, 1, 1, 0, 2)
PIECE_Y = (0, 1, 0, 1, 2, 0)


def field_rows(x):
    one = jnp.ones_like(x[0])
    rows = []
    for c in range(3):
        part = pieces(x[c], 3)
        rows += [part[j] for j in PIECE_X]
    rows += pieces(dot3(x, x) + core_radius**2, 3)
    rows += [one, one, one]
    return rows


def source_rows(y):
    one = jnp.ones_like(y[0])
    rows = []
    for c in range(3):
        part = pieces(-2.0 * y[c], 3)
        rows += [part[j] for j in PIECE_Y]
    rows += [one, one, one]
    rows += pieces(dot3(y, y), 3)
    return rows


def kernel(
    mid_ref, line_ref, burg_ref, cell_ref, node_ref, glist, gcount, plist, pcount,
    nout_ref, cout_ref,
    S, own, pkt, ghost, feat, FT, yrow, YT, xrow, XB, R2, VS, MT, mono, bl, cacc, cpkt, crecv,
    frow, nacc, npkt, nrecv, send_sem, recv_sem,
):
    i = lax.axis_index("dx")
    j = lax.axis_index("dy")
    ndx = lax.axis_size("dx")
    ndy = lax.axis_size("dy")
    peers = [
        (lax.rem(i + (a + ndx), ndx), lax.rem(j + (b + ndy), ndy)) for a, b in neighbour_offsets
    ]

    barrier = pltpu.get_barrier_semaphore()
    for peer in peers:
        pl.semaphore_signal(barrier, inc=1, device_id=peer, device_id_type=MESH)

    def sends(kind, source, target):
        copies = []
        for k in range(8):
            copies.append(
                pltpu.make_async_remote_copy(
                    src_ref=source(k),
                    dst_ref=target.at[7 - k],
                    send_sem=send_sem.at[kind, k],
                    recv_sem=recv_sem.at[kind, 7 - k],
                    device_id=peers[k],
                    device_id_type=MESH,
                )
            )
        return copies

    for t in range(TILES):
        window = pl.ds(t * TILE, TILE)
        for first, ref in ((0, mid_ref), (3, line_ref), (6, burg_ref)):
            values = ref[0, 0, :, window]
            S[first : first + 3, t, :] = values
            own[t, first : first + 3, :] = values
    for k in range(8):
        for g in range(GHOST):
            valid = jnp.minimum(jnp.maximum(gcount[0, 0, k] - g, 0), 1).astype(f32)
            pkt[k, :, g, :] = own[glist[0, 0, k, g]] * valid

    ghost_copies = sends(0, lambda k: pkt.at[k], ghost)
    zero_rows = jnp.zeros((AUG, TILE), f32)

    def prepare_sources(first, count):
        rows = pl.ds(first, count)
        y = [S[c, rows, :] - 0.5 for c in range(3)]
        line = [S[3 + c, rows, :] for c in range(3)]
        burgers = [S[6 + c, rows, :] for c in range(3)]
        for index, value in enumerate(source_features(y, line, burgers)):
            feat[rows, index, :] = value
        for index, value in enumerate(source_rows(y)):
            yrow[rows, index, :] = value
        zero = jnp.zeros_like(y[0])
        for index in range(36, FEATURES):
            feat[rows, index, :] = zero
        for index in range(24, AUG):
            yrow[rows, index, :] = zero

        def per_tile(t, carry):
            FT[t] = jnp.concatenate(pieces(feat[t], 3), axis=0).astype(bf16)
            rows_t = yrow[t]
            YT[0, t] = jnp.concatenate([rows_t, zero_rows], axis=0).T.astype(bf16)
            YT[1, t] = jnp.concatenate([zero_rows, rows_t], axis=0).T.astype(bf16)
            return carry

        lax.fori_loop(first, first + count, per_tile, 0, unroll=4)

    prepare_sources(0, TILES)

    own_x = [S[c, 0:TILES, :] - 0.5 for c in range(3)]
    field = field_rows(own_x)
    for index, value in enumerate(field):
        xrow[:, index, :] = value
    for index in range(len(field), AUG):
        xrow[:, index, :] = jnp.zeros((TILES, TILE), f32)

    def field_tile(t, carry):
        rows_t = xrow[t]
        left = jnp.concatenate([rows_t, zero_rows], axis=0)
        right = jnp.concatenate([zero_rows, rows_t], axis=0)
        XB[t] = jnp.concatenate([left, right], axis=1).astype(bf16)
        return carry

    lax.fori_loop(0, TILES, field_tile, 0, unroll=4)
    FT[POOL] = jnp.zeros((3 * FEATURES, TILE), bf16)

    pl.semaphore_wait(barrier, 8)
    for copy in ghost_copies:
        copy.start()

    scaled = [2.0 * (S[c, 0:TILES, :] - 0.5) for c in range(3)]
    powers = []
    for u in scaled:
        square = u * u
        powers.append([jnp.ones_like(u), u, square, square * u, square * square])
    for r, (e0, e1, e2) in enumerate(exponent_table()):
        mono[:, r, :] = powers[0][e0] * powers[1][e1] * powers[2][e2]
    for r in range(35, 40):
        mono[:, r, :] = jnp.zeros((TILES, TILE), f32)
    for beta in range(3):
        for gamma in range(3):
            bl[:, 3 * beta + gamma, :] = S[6 + beta, 0:TILES, :] * S[3 + gamma, 0:TILES, :]
    cacc[...] = jnp.zeros_like(cacc)
    sub128 = lax.broadcasted_iota(jnp.int32, (TILE, TILE), 0)

    def cell_group(group, carry):
        highs, lows, members = [], [], []
        for inner in range(4):
            t = group * 4 + inner
            mono_t = mono[t]
            bl_t = bl[t]
            block = [bl_t[k : k + 1, :] * mono_t for k in range(9)]
            block.append(jnp.zeros((8, TILE), f32))
            terms = jnp.concatenate(block, axis=0)
            high = terms.astype(bf16)
            highs.append(high)
            lows.append((terms - high.astype(f32)).astype(bf16))
            cells = cell_ref[0, :, pl.ds(pl.multiple_of(t * TILE, TILE), TILE)]
            members.append(jnp.where(sub128 == cells, 1.0, 0.0).astype(bf16))
        lhs = jnp.concatenate(
            [jnp.concatenate(highs, axis=1), jnp.concatenate(lows, axis=1)], axis=0
        )
        rhs = jnp.concatenate(members, axis=1)
        cacc[...] += lax.dot_general(lhs, rhs, NT, preferred_element_type=f32)
        return carry

    lax.fori_loop(0, TILES // 4, cell_group, 0)
    for block in range(3):
        rows = min(TILE, TERMS - block * TILE)
        part = cacc[block * TILE : block * TILE + rows, :] + cacc[TERMS + block * TILE : TERMS + block * TILE + rows, :]
        if rows < TILE:
            part = jnp.concatenate([part, jnp.zeros((TILE - rows, TILE), f32)], axis=0)
        turned = part.T
        for d in range(9):
            cpkt[d, :, block * TILE : (block + 1) * TILE] = turned[8 * d : 8 * d + 8, :]
    cell_copies = sends(1, lambda k: cpkt.at[k + (k >= 4)], crecv)
    for copy in cell_copies:
        copy.start()

    for k in range(8):
        ghost_copies[k].wait()
    for q in range(8):
        a, b = neighbour_offsets[q]
        rows = pl.ds(TILES + GHOST * q, GHOST)
        S[0, rows, :] = ghost[q, 0] + float(a)
        S[1, rows, :] = ghost[q, 1] + float(b)
        for c in range(2, 9):
            S[c, rows, :] = ghost[q, c]
    prepare_sources(TILES, POOL - TILES)

    def stage_inner(t):
        rhs = XB[t]
        for pair in range(NP // 2):
            lhs = YT[0, plist[0, 0, t, 2 * pair]] + YT[1, plist[0, 0, t, 2 * pair + 1]]
            R2[pair] = jnp.dot(lhs, rhs, preferred_element_type=f32)

    def stage_power():
        for n in range(NP):
            radius_sq = R2[n // 2, :, (n % 2) * TILE : (n % 2 + 1) * TILE]
            inverse = lax.rsqrt(radius_sq)
            square = inverse * inverse
            value = square * square * inverse
            high = value.astype(bf16)
            VS[n * TILE : (n + 1) * TILE, 0:TILE] = high
            VS[n * TILE : (n + 1) * TILE, TILE : 2 * TILE] = (value - high.astype(f32)).astype(bf16)

    def stage_sum(t):
        count = pcount[0, 0, t]
        chosen = []
        for n in range(NP):
            valid = jnp.minimum(jnp.maximum(count - n, 0), 1)
            chosen.append(FT[valid * (plist[0, 0, t, n] - POOL) + POOL])
        total = jnp.dot(jnp.concatenate(chosen, axis=1), VS[...], preferred_element_type=f32)
        total = total[:, 0:TILE] + total[:, TILE : 2 * TILE]
        MT[t] = total[0:FEATURES] + total[FEATURES : 2 * FEATURES] + total[2 * FEATURES : 3 * FEATURES]

    stage_inner(0)
    stage_power()
    stage_inner(1)

    def pair_step(t, carry):
        stage_sum(t - 2)
        stage_power()
        stage_inner(t)
        return carry

    lax.fori_loop(2, TILES, pair_step, 0)
    stage_sum(TILES - 2)
    stage_power()
    stage_sum(TILES - 1)

    x = [S[c, 0:TILES, :] - 0.5 for c in range(3)]
    stress = stress_from_moments(x, [MT[:, r, :] for r in range(36)])
    burgers = [S[6 + c, 0:TILES, :] for c in range(3)]
    line = [S[3 + c, 0:TILES, :] for c in range(3)]
    traction = [dot3([stress[SYM[(m, n)]] for n in range(3)], burgers) for m in range(3)]
    force = cross(traction, line)
    for c in range(3):
        for piece, value in enumerate(pieces(0.5 * force[c], 2)):
            frow[:, 2 * c + piece, :] = value
    nacc[...] = jnp.zeros_like(nacc)
    sub40 = lax.broadcasted_iota(jnp.int32, (40, TILE), 0)

    def node_group(group, carry):
        lefts, rights = [], []
        for inner in range(4):
            t = group * 4 + inner
            rows_t = frow[t]
            for end in range(2):
                nodes = node_ref[0, 0, end : end + 1, pl.ds(pl.multiple_of(t * TILE, TILE), TILE)]
                outer = sub40 == lax.shift_right_logical(nodes, 7)
                lefts.append(
                    jnp.concatenate(
                        [jnp.where(outer, rows_t[r : r + 1, :], 0.0) for r in range(6)], axis=0
                    ).astype(bf16)
                )
                rights.append(jnp.where(sub128 == (nodes & 127), 1.0, 0.0).astype(bf16))
        nacc[...] += lax.dot_general(
            jnp.concatenate(lefts, axis=1),
            jnp.concatenate(rights, axis=1),
            NT,
            preferred_element_type=f32,
        )
        return carry

    lax.fori_loop(0, TILES // 4, node_group, 0)
    for c in range(3):
        total = nacc[80 * c : 80 * c + 40, :] + nacc[80 * c + 40 : 80 * c + 80, :]
        for d in range(9):
            npkt[d, c] = total[4 * d : 4 * d + 4, :]
    node_copies = sends(2, lambda k: npkt.at[k + (k >= 4)], nrecv)
    for copy in node_copies:
        copy.start()

    for copy in cell_copies:
        copy.wait()
    moments = cpkt[4]
    for q in range(8):
        moments = moments + crecv[q]
    turned = []
    for block in range(3):
        part = moments[:, block * TILE : (block + 1) * TILE]
        part = jnp.concatenate([part, jnp.zeros((TILE - CELL_DEV, TILE), f32)], axis=0)
        turned.append(part.T)
    turned = jnp.concatenate(turned, axis=0)
    for k in range(9):
        cout_ref[35 * k : 35 * k + 35, :] = turned[40 * k : 40 * k + 35, 0:CELL_DEV]
    for copy in node_copies:
        copy.wait()
    nodes = npkt[4]
    for q in range(8):
        nodes = nodes + nrecv[q]
    for quarter in range(4):
        nout_ref[0, 0, :, quarter * TILE : (quarter + 1) * TILE] = nodes[:, quarter, :]


def on_device(*arguments):
    vmem = pl.BlockSpec(memory_space=pltpu.VMEM)
    smem = pl.BlockSpec(memory_space=pltpu.SMEM)
    return pl.pallas_call(
        kernel,
        out_shape=(
            jax.ShapeDtypeStruct((1, 1, 3, NODE_DEV), f32),
            jax.ShapeDtypeStruct((COMPONENTS, CELL_DEV), f32),
        ),
        in_specs=[vmem] * 5 + [smem] * 4,
        out_specs=(vmem, vmem),
        scratch_shapes=[
            pltpu.VMEM((9, POOL, TILE), f32),
            pltpu.VMEM((TILES, 9, TILE), f32),
            pltpu.VMEM((8, 9, GHOST, TILE), f32),
            pltpu.VMEM((8, 9, GHOST, TILE), f32),
            pltpu.VMEM((POOL, FEATURES, TILE), f32),
            pltpu.VMEM((POOL + 1, 3 * FEATURES, TILE), bf16),
            pltpu.VMEM((POOL, AUG, TILE), f32),
            pltpu.VMEM((2, POOL, TILE, 2 * AUG), bf16),
            pltpu.VMEM((TILES, AUG, TILE), f32),
            pltpu.VMEM((TILES, 2 * AUG, 2 * TILE), bf16),
            pltpu.VMEM((NP // 2, TILE, 2 * TILE), f32),
            pltpu.VMEM((NP * TILE, 2 * TILE), bf16),
            pltpu.VMEM((TILES, FEATURES, TILE), f32),
            pltpu.VMEM((TILES, 40, TILE), f32),
            pltpu.VMEM((TILES, 16, TILE), f32),
            pltpu.VMEM((2 * TERMS, TILE), f32),
            pltpu.VMEM((9, CELL_DEV, 384), f32),
            pltpu.VMEM((8, CELL_DEV, 384), f32),
            pltpu.VMEM((TILES, 8, TILE), f32),
            pltpu.VMEM((240, TILE), f32),
            pltpu.VMEM((9, 3, 4, TILE), f32),
            pltpu.VMEM((8, 3, 4, TILE), f32),
            pltpu.SemaphoreType.DMA((3, 8)),
            pltpu.SemaphoreType.DMA((3, 8)),
        ],
        compiler_params=pltpu.CompilerParams(collective_id=0, has_side_effects=True, vmem_limit_bytes=48 * 1024 * 1024),
        name="segments",
    )(*arguments)


def solution(mesh):
    in_specs = (
        P("dx", "dy", None, None),
        P("dx", "dy", None, None),
        P("dx", "dy", None, None),
        P("dx", "dy", None),
        P("dx", "dy", None, None),
        P("dx", "dy", None, None),
        P("dx", "dy", None),
        P("dx", "dy", None, None),
        P("dx", "dy", None),
    )
    out_specs = (P("dx", "dy", None, None), P(None, ("dx", "dy")))
    return jax.shard_map(
        on_device, mesh=mesh, in_specs=in_specs, out_specs=out_specs, check_vma=False
    )
```

```python
import jax
import jax.numpy as jnp
from jax import lax
from jax.experimental import pallas as pl
from jax.experimental.pallas import tpu as pltpu
from jax.sharding import PartitionSpec as P

TILE = 128
TILES = 32
GHOST = 2
NP = 12
NODE_DEV = 512
CELL_DEV = 8
COMPONENTS = 315
POOL = 48
FEATURES = 40
AUG = 32
UNROLL = 6
NODE_GROUP = 16
TERMS = 368

core_radius = 0.1
shear_scale = 0.25
neighbour_offsets = ((-1, -1), (-1, 0), (-1, 1), (0, -1), (0, 1), (1, -1), (1, 0), (1, 1))
f32 = jnp.float32
bf16 = jnp.bfloat16
MESH = pl.DeviceIdType.MESH
NT = (((1,), (1,)), ((), ()))


def rounded(value):
    return value.astype(bf16).astype(f32)


def pieces(value, count):
    parts = []
    for _ in range(count - 1):
        part = rounded(value)
        parts.append(part)
        value = value - part
    parts.append(rounded(value))
    return parts


def each_tile(ref, index, first=0, count=TILES):
    blocks, pitch, lanes = ref.shape
    return ref.reshape(blocks * pitch, lanes).at[pl.ds(first * pitch + index, count, stride=pitch), :]


def exponent_table():
    exponent_rows = []
    for degree in range(5):
        for first_power in range(degree, -1, -1):
            for second in range(degree - first_power, -1, -1):
                exponent_rows.append((first_power, second, degree - first_power - second))
    return exponent_rows


def cross(u, v):
    return [
        u[1] * v[2] - u[2] * v[1],
        u[2] * v[0] - u[0] * v[2],
        u[0] * v[1] - u[1] * v[0],
    ]


def dot3(u, v):
    return u[0] * v[0] + u[1] * v[1] + u[2] * v[2]


PAIRS6 = ((0, 0), (1, 1), (2, 2), (0, 1), (0, 2), (1, 2))
SYM = {}
for _slot, (_m, _n) in enumerate(PAIRS6):
    SYM[(_m, _n)] = _slot
    SYM[(_n, _m)] = _slot


def source_features(y, line, burgers):
    g = [shear_scale * v for v in cross(burgers, line)]
    h = [[y[k] * g[n] for n in range(3)] for k in range(3)]
    q = [[y[k] * h[l][n] for n in range(3)] for (k, l) in PAIRS6]
    y2 = dot3(y, y)
    trace = h[0][0] + h[1][1] + h[2][2]
    c = []
    for m, n in PAIRS6:
        value = y2 * (h[m][n] + h[n][m]) - 3.0 * trace * (y[m] * y[n])
        if m == n:
            value = value + y2 * trace
        c.append(value)
    rows = list(g)
    for k in range(3):
        rows += h[k]
    for kl in range(6):
        rows += q[kl]
    rows += c
    return rows


def stress_from_moments(x, moment):
    c2 = core_radius**2
    G = moment[0:3]
    H = [moment[3 + 3 * k : 6 + 3 * k] for k in range(3)]
    Q = [moment[12 + 3 * kl : 15 + 3 * kl] for kl in range(6)]
    C = moment[30:36]
    x2 = dot3(x, x)
    xG = dot3(x, G)
    trH = H[0][0] + H[1][1] + H[2][2]
    Z = [Q[0][n] + Q[1][n] + Q[2][n] for n in range(3)]
    W = [Q[SYM[(0, n)]][0] + Q[SYM[(1, n)]][1] + Q[SYM[(2, n)]][2] for n in range(3)]
    xH = [x[0] * H[0][n] + x[1] * H[1][n] + x[2] * H[2][n] for n in range(3)]
    Hx = [H[n][0] * x[0] + H[n][1] * x[1] + H[n][2] * x[2] for n in range(3)]
    xQ = [
        [x[0] * Q[SYM[(0, m)]][n] + x[1] * Q[SYM[(1, m)]][n] + x[2] * Q[SYM[(2, m)]][n] for n in range(3)]
        for m in range(3)
    ]
    lead = [(x2 + c2) * G[n] - 2.0 * xH[n] + Z[n] + 3.0 * Hx[n] - 3.0 * W[n] for n in range(3)]
    both = xG - trH
    diagonal = (
        (x2 + 2.5 * c2) * both
        - 2.0 * dot3(x, xH)
        + 2.0 * dot3(x, W)
        + dot3(x, Z)
    )
    out = []
    for m, n in PAIRS6:
        value = (
            x[m] * lead[n]
            + x[n] * lead[m]
            - (x2 + c2) * (H[m][n] + H[n][m])
            + 2.0 * (xQ[m][n] + xQ[n][m])
            - 3.0 * (x[m] * x[n] * both + dot3(x, Q[SYM[(m, n)]]))
            - C[SYM[(m, n)]]
        )
        if m == n:
            value = value + diagonal
        out.append(value)
    return out


PIECE_X = (0, 0, 1, 1, 0, 2)
PIECE_Y = (0, 1, 0, 1, 2, 0)


def field_rows(x):
    one = jnp.ones_like(x[0])
    rows = []
    for c in range(3):
        part = pieces(x[c], 3)
        rows += [part[j] for j in PIECE_X]
    rows += pieces(dot3(x, x) + core_radius**2, 3)
    rows += [one, one, one]
    return rows


def source_rows(y):
    one = jnp.ones_like(y[0])
    rows = []
    for c in range(3):
        part = pieces(-2.0 * y[c], 3)
        rows += [part[j] for j in PIECE_Y]
    rows += [one, one, one]
    rows += pieces(dot3(y, y), 3)
    return rows


def kernel(
    mid_any, line_any, burg_any, cell_any, node_any, glist_any, gcount_any, plist_any, pcount_any,
    nout_ref, cout_ref,
    mid, line, burg, cells_in, nodes_in, glist, gcount, plist, pcount,
    own, pkt, ghost, far, feat, FT, yrow, YT, xrow, XL, XR, R2, VH, VL, MT, mono, bl, cacc, cpkt,
    crecv, frow, nacc, npkt, nrecv, send_sem, recv_sem, load_sem,
):
    i = lax.axis_index("dx")
    j = lax.axis_index("dy")
    ndx = lax.axis_size("dx")
    ndy = lax.axis_size("dy")
    peers = [
        (lax.rem(i + (a + ndx), ndx), lax.rem(j + (b + ndy), ndy)) for a, b in neighbour_offsets
    ]

    barrier = pltpu.get_barrier_semaphore()
    for peer in peers:
        pl.semaphore_signal(barrier, inc=1, device_id=peer, device_id_type=MESH)

    def sends(kind, source, target):
        copies = []
        for k in range(8):
            copies.append(
                pltpu.make_async_remote_copy(
                    src_ref=source(k),
                    dst_ref=target.at[7 - k],
                    send_sem=send_sem.at[kind, k],
                    recv_sem=recv_sem.at[kind, 7 - k],
                    device_id=peers[k],
                    device_id_type=MESH,
                )
            )
        return copies

    loads = [
        pltpu.make_async_copy(source, target, load_sem.at[index])
        for index, (source, target) in enumerate(
            (
                (glist_any, glist),
                (gcount_any, gcount),
                (mid_any, mid),
                (line_any, line),
                (burg_any, burg),
                (plist_any, plist),
                (pcount_any, pcount),
                (cell_any, cells_in),
                (node_any, nodes_in),
            )
        )
    ]
    for load in loads:
        load.start()
    for load in loads:
        load.wait()

    for c in range(3):
        each_tile(own, c)[...] = mid[c]
        each_tile(own, 3 + c)[...] = line[c]
        each_tile(own, 6 + c)[...] = burg[c]
    for k in range(8):
        for g in range(GHOST):
            valid = jnp.minimum(jnp.maximum(gcount[0, 0, k] - g, 0), 1).astype(f32)
            pkt[k, :, g, :] = own[glist[g, k]][0:9] * valid

    ghost_copies = sends(0, lambda k: pkt.at[k], ghost)
    zero_rows = jnp.zeros((AUG, TILE), f32)

    def prepare_sources(first, count, y, line_rows, burgers, unroll):
        for index, value in enumerate(source_features(y, line_rows, burgers)):
            each_tile(feat, index, first, count)[...] = value
        for index, value in enumerate(source_rows(y)):
            each_tile(yrow, index, first, count)[...] = value
        zero = jnp.zeros_like(y[0])
        for index in range(36, FEATURES):
            each_tile(feat, index, first, count)[...] = zero
        for index in range(24, AUG):
            each_tile(yrow, index, first, count)[...] = zero

        def per_tile(t, carry):
            FT[t] = jnp.concatenate(pieces(feat[t], 3), axis=0).astype(bf16)
            rows_t = yrow[t]
            YT[0, t] = jnp.concatenate([rows_t, zero_rows], axis=0).astype(bf16).T
            YT[1, t] = jnp.concatenate([zero_rows, rows_t], axis=0).astype(bf16).T
            return carry

        lax.fori_loop(first, first + count, per_tile, 0, unroll=unroll)

    own_x = [mid[c] - 0.5 for c in range(3)]
    own_line = [line[c] for c in range(3)]
    own_burgers = [burg[c] for c in range(3)]
    prepare_sources(0, TILES, own_x, own_line, own_burgers, 8)

    field = field_rows(own_x)
    for index, value in enumerate(field):
        each_tile(xrow, index)[...] = value
    for index in range(len(field), AUG):
        each_tile(xrow, index)[...] = jnp.zeros((TILES, TILE), f32)

    def field_tile(t, carry):
        rows_t = xrow[t]
        XL[t] = jnp.concatenate([rows_t, zero_rows], axis=0).astype(bf16)
        XR[t] = jnp.concatenate([zero_rows, rows_t], axis=0).astype(bf16)
        return carry

    lax.fori_loop(0, TILES, field_tile, 0, unroll=8)
    FT[POOL] = jnp.zeros((3 * FEATURES, TILE), bf16)

    pl.semaphore_wait(barrier, 8)
    for copy in ghost_copies:
        copy.start()

    scaled = [2.0 * (mid[c] - 0.5) for c in range(3)]
    powers = []
    for u in scaled:
        square = u * u
        powers.append([jnp.ones_like(u), u, square, square * u, square * square])
    for r, (e0, e1, e2) in enumerate(exponent_table()):
        each_tile(mono, r)[...] = powers[0][e0] * powers[1][e1] * powers[2][e2]
    for r in range(35, 40):
        each_tile(mono, r)[...] = jnp.zeros((TILES, TILE), f32)
    for beta in range(3):
        for gamma in range(3):
            each_tile(bl, 3 * beta + gamma)[...] = burg[beta] * line[gamma]
    cacc[...] = jnp.zeros_like(cacc)
    sub128 = lax.broadcasted_iota(jnp.int32, (TILE, TILE), 0)

    def cell_group(group, carry):
        highs, lows, members = [], [], []
        for inner in range(4):
            t = group * 4 + inner
            mono_t = mono[t]
            bl_t = bl[t]
            block = [bl_t[k : k + 1, :] * mono_t for k in range(9)]
            block.append(jnp.zeros((8, TILE), f32))
            terms = jnp.concatenate(block, axis=0)
            high = terms.astype(bf16)
            highs.append(high)
            lows.append((terms - high.astype(f32)).astype(bf16))
            cells = cells_in[pl.ds(t, 1), :]
            members.append(jnp.where(sub128 == cells, 1.0, 0.0).astype(bf16))
        lhs = jnp.concatenate(
            [jnp.concatenate(highs, axis=1), jnp.concatenate(lows, axis=1)], axis=0
        )
        rhs = jnp.concatenate(members, axis=1)
        cacc[...] += lax.dot_general(lhs, rhs, NT, preferred_element_type=f32)
        return carry

    lax.fori_loop(0, TILES // 4, cell_group, 0)
    for block in range(3):
        rows = min(TILE, TERMS - block * TILE)
        part = cacc[block * TILE : block * TILE + rows, :] + cacc[TERMS + block * TILE : TERMS + block * TILE + rows, :]
        if rows < TILE:
            part = jnp.concatenate([part, jnp.zeros((TILE - rows, TILE), f32)], axis=0)
        turned = part.T
        for d in range(9):
            cpkt[d, :, block * TILE : (block + 1) * TILE] = turned[8 * d : 8 * d + 8, :]
    cell_copies = sends(1, lambda k: cpkt.at[k + (k >= 4)], crecv)
    for copy in cell_copies:
        copy.start()

    for k in range(8):
        ghost_copies[k].wait()
    for q in range(8):
        a, b = neighbour_offsets[q]
        rows = pl.ds(GHOST * q, GHOST)
        far[0, rows, :] = ghost[q, 0] + float(a)
        far[1, rows, :] = ghost[q, 1] + float(b)
        for c in range(2, 9):
            far[c, rows, :] = ghost[q, c]
    prepare_sources(
        TILES,
        POOL - TILES,
        [far[c] - 0.5 for c in range(3)],
        [far[c] for c in range(3, 6)],
        [far[c] for c in range(6, 9)],
        8,
    )

    def stage_inner(t, slot):
        rhs = jnp.concatenate([XL[t], XR[t]], axis=1)
        for pair in range(NP // 2):
            lhs = YT[0, plist[2 * pair, 0, t]] + YT[1, plist[2 * pair + 1, 0, t]]
            R2[slot, pair] = jnp.dot(lhs, rhs, preferred_element_type=f32)

    def stage_power(slot):
        for n in range(NP):
            radius_sq = R2[slot, n // 2, :, (n % 2) * TILE : (n % 2 + 1) * TILE]
            inverse = lax.rsqrt(radius_sq)
            square = inverse * inverse
            value = square * square * inverse
            high = value.astype(bf16)
            VH[slot, n * TILE : (n + 1) * TILE, :] = high
            VL[slot, n * TILE : (n + 1) * TILE, :] = (value - high.astype(f32)).astype(bf16)

    def stage_sum(t, slot):
        count = pcount[0, 0, t]
        chosen = []
        for n in range(NP):
            valid = jnp.minimum(jnp.maximum(count - n, 0), 1)
            chosen.append(FT[valid * (plist[n, 0, t] - POOL) + POOL])
        weights = jnp.concatenate([VH[slot], VL[slot]], axis=1)
        total = jnp.dot(jnp.concatenate(chosen, axis=1), weights, preferred_element_type=f32)
        total = total[:, 0:TILE] + total[:, TILE : 2 * TILE]
        MT[t] = total[0:FEATURES] + total[FEATURES : 2 * FEATURES] + total[2 * FEATURES : 3 * FEATURES]

    stage_inner(0, 0)
    stage_power(0)
    stage_inner(1, 1)

    def pair_steps(step, carry):
        for inner in range(UNROLL):
            t = step * UNROLL + inner + 2
            stage_sum(t - 2, inner % 2)
            stage_power((inner + 1) % 2)
            stage_inner(t, inner % 2)
        return carry

    lax.fori_loop(0, (TILES - 2) // UNROLL, pair_steps, 0)
    stage_sum(TILES - 2, 0)
    stage_power(1)
    stage_sum(TILES - 1, 1)

    own_x = [mid[c] - 0.5 for c in range(3)]
    own_line = [line[c] for c in range(3)]
    own_burgers = [burg[c] for c in range(3)]
    stress = stress_from_moments(own_x, [each_tile(MT, r)[...] for r in range(36)])
    traction = [dot3([stress[SYM[(m, n)]] for n in range(3)], own_burgers) for m in range(3)]
    force = cross(traction, own_line)
    for c in range(3):
        for piece, value in enumerate(pieces(0.5 * force[c], 2)):
            each_tile(frow, 2 * c + piece)[...] = value
    nacc[...] = jnp.zeros_like(nacc)
    sub40 = lax.broadcasted_iota(jnp.int32, (40, TILE), 0)

    def node_group(group, carry):
        lefts, rights = [], []
        for inner in range(NODE_GROUP):
            t = group * NODE_GROUP + inner
            rows_t = frow[t]
            ends = nodes_in[t]
            for end in range(2):
                nodes = ends[end : end + 1, :]
                outer = sub40 == lax.shift_right_logical(nodes, 7)
                lefts.append(
                    jnp.concatenate(
                        [jnp.where(outer, rows_t[r : r + 1, :], 0.0) for r in range(6)], axis=0
                    ).astype(bf16)
                )
                rights.append(jnp.where(sub128 == (nodes & 127), 1.0, 0.0).astype(bf16))
        nacc[...] += lax.dot_general(
            jnp.concatenate(lefts, axis=1),
            jnp.concatenate(rights, axis=1),
            NT,
            preferred_element_type=f32,
        )
        return carry

    lax.fori_loop(0, TILES // NODE_GROUP, node_group, 0)
    for c in range(3):
        total = nacc[80 * c : 80 * c + 40, :] + nacc[80 * c + 40 : 80 * c + 80, :]
        for d in range(9):
            npkt[d, c] = total[4 * d : 4 * d + 4, :]
    node_copies = sends(2, lambda k: npkt.at[k + (k >= 4)], nrecv)
    for copy in node_copies:
        copy.start()

    for copy in cell_copies:
        copy.wait()
    moments = cpkt[4]
    for q in range(8):
        moments = moments + crecv[q]
    for k in range(9):
        cout_ref[:, 35 * k : 35 * k + 35] = moments[:, 40 * k : 40 * k + 35]
    for copy in node_copies:
        copy.wait()
    nodes = npkt[4]
    for q in range(8):
        nodes = nodes + nrecv[q]
    nout_ref[...] = nodes


def on_device(
    seg_mid, seg_line, seg_burgers, seg_cell, seg_node, ghost_list, ghost_count, pair_list, pair_count
):
    shape3 = (3, TILES, TILE)
    arguments = (
        seg_mid.reshape(shape3),
        seg_line.reshape(shape3),
        seg_burgers.reshape(shape3),
        seg_cell.reshape(TILES, TILE),
        seg_node.reshape(2, TILES, TILE).transpose(1, 0, 2),
        ghost_list.reshape(8, GHOST).T,
        ghost_count,
        pair_list.transpose(3, 0, 1, 2).reshape(NP, 1, TILES),
        pair_count,
    )
    vmem = pl.BlockSpec(memory_space=pltpu.VMEM)
    anywhere = pl.BlockSpec(memory_space=pl.ANY)
    node_force, moments = pl.pallas_call(
        kernel,
        out_shape=(
            jax.ShapeDtypeStruct((3, NODE_DEV // TILE, TILE), f32),
            jax.ShapeDtypeStruct((CELL_DEV, COMPONENTS), f32),
        ),
        in_specs=[anywhere] * 9,
        out_specs=(vmem, vmem),
        scratch_shapes=[
            pltpu.VMEM(shape3, f32),
            pltpu.VMEM(shape3, f32),
            pltpu.VMEM(shape3, f32),
            pltpu.VMEM((TILES, TILE), jnp.int32),
            pltpu.VMEM((TILES, 2, TILE), jnp.int32),
            pltpu.SMEM((GHOST, 8), jnp.int32),
            pltpu.SMEM((1, 1, 8), jnp.int32),
            pltpu.SMEM((NP, 1, TILES), jnp.int32),
            pltpu.SMEM((1, 1, TILES), jnp.int32),
            pltpu.VMEM((TILES, 16, TILE), f32),
            pltpu.VMEM((8, 9, GHOST, TILE), f32),
            pltpu.VMEM((8, 9, GHOST, TILE), f32),
            pltpu.VMEM((9, POOL - TILES, TILE), f32),
            pltpu.VMEM((POOL, FEATURES, TILE), f32),
            pltpu.VMEM((POOL + 1, 3 * FEATURES, TILE), bf16),
            pltpu.VMEM((POOL, AUG, TILE), f32),
            pltpu.VMEM((2, POOL, TILE, 2 * AUG), bf16),
            pltpu.VMEM((TILES, AUG, TILE), f32),
            pltpu.VMEM((TILES, 2 * AUG, TILE), bf16),
            pltpu.VMEM((TILES, 2 * AUG, TILE), bf16),
            pltpu.VMEM((2, NP // 2, TILE, 2 * TILE), f32),
            pltpu.VMEM((2, NP * TILE, TILE), bf16),
            pltpu.VMEM((2, NP * TILE, TILE), bf16),
            pltpu.VMEM((TILES, FEATURES, TILE), f32),
            pltpu.VMEM((TILES, 40, TILE), f32),
            pltpu.VMEM((TILES, 16, TILE), f32),
            pltpu.VMEM((2 * TERMS, TILE), f32),
            pltpu.VMEM((9, CELL_DEV, 384), f32),
            pltpu.VMEM((8, CELL_DEV, 384), f32),
            pltpu.VMEM((TILES, 8, TILE), f32),
            pltpu.VMEM((240, TILE), f32),
            pltpu.VMEM((9, 3, 4, TILE), f32),
            pltpu.VMEM((8, 3, 4, TILE), f32),
            pltpu.SemaphoreType.DMA((3, 8)),
            pltpu.SemaphoreType.DMA((3, 8)),
            pltpu.SemaphoreType.DMA((9,)),
        ],
        compiler_params=pltpu.CompilerParams(
            collective_id=0, has_side_effects=True, vmem_limit_bytes=60 * 1024 * 1024
        ),
        name="segments",
    )(*arguments)
    return node_force.reshape(1, 1, 3, NODE_DEV), moments.T


def solution(mesh):
    in_specs = (
        P("dx", "dy", None, None),
        P("dx", "dy", None, None),
        P("dx", "dy", None, None),
        P("dx", "dy", None),
        P("dx", "dy", None, None),
        P("dx", "dy", None, None),
        P("dx", "dy", None),
        P("dx", "dy", None, None),
        P("dx", "dy", None),
    )
    out_specs = (P("dx", "dy", None, None), P(None, ("dx", "dy")))
    return jax.shard_map(
        on_device, mesh=mesh, in_specs=in_specs, out_specs=out_specs, check_vma=False
    )
```

```python
import jax
import jax.numpy as jnp
from jax import lax
from jax.experimental import pallas as pl
from jax.experimental.pallas import tpu as pltpu
from jax.sharding import PartitionSpec as P

TILE = 128
TILES = 32
GHOST = 2
NP = 12
NODE_DEV = 512
CELL_DEV = 8
COMPONENTS = 315
POOL = 48
FEATURES = 40
AUG = 32
UNROLL = 10
NODE_GROUP = 16
TERMS = 368

core_radius = 0.1
shear_scale = 0.25
neighbour_offsets = ((-1, -1), (-1, 0), (-1, 1), (0, -1), (0, 1), (1, -1), (1, 0), (1, 1))
f32 = jnp.float32
bf16 = jnp.bfloat16
MESH = pl.DeviceIdType.MESH
NT = (((1,), (1,)), ((), ()))


def rounded(value):
    return value.astype(bf16).astype(f32)


def pieces(value, count):
    parts = []
    for _ in range(count - 1):
        part = rounded(value)
        parts.append(part)
        value = value - part
    parts.append(rounded(value))
    return parts


def each_tile(ref, pitch, index, first=0, count=TILES):
    return ref.at[pl.ds(first * pitch + index, count, stride=pitch), :]


def tile_rows(ref, pitch, t, rows):
    return ref.at[pl.ds(t * pitch, rows), :]


def exponent_table():
    exponent_rows = []
    for degree in range(5):
        for first_power in range(degree, -1, -1):
            for second in range(degree - first_power, -1, -1):
                exponent_rows.append((first_power, second, degree - first_power - second))
    return exponent_rows


def cross(u, v):
    return [
        u[1] * v[2] - u[2] * v[1],
        u[2] * v[0] - u[0] * v[2],
        u[0] * v[1] - u[1] * v[0],
    ]


def dot3(u, v):
    return u[0] * v[0] + u[1] * v[1] + u[2] * v[2]


PAIRS6 = ((0, 0), (1, 1), (2, 2), (0, 1), (0, 2), (1, 2))
SYM = {}
for _slot, (_m, _n) in enumerate(PAIRS6):
    SYM[(_m, _n)] = _slot
    SYM[(_n, _m)] = _slot


def source_features(y, line, burgers):
    g = [shear_scale * v for v in cross(burgers, line)]
    h = [[y[k] * g[n] for n in range(3)] for k in range(3)]
    q = [[y[k] * h[l][n] for n in range(3)] for (k, l) in PAIRS6]
    y2 = dot3(y, y)
    trace = h[0][0] + h[1][1] + h[2][2]
    c = []
    for m, n in PAIRS6:
        value = y2 * (h[m][n] + h[n][m]) - 3.0 * trace * (y[m] * y[n])
        if m == n:
            value = value + y2 * trace
        c.append(value)
    rows = list(g)
    for k in range(3):
        rows += h[k]
    for kl in range(6):
        rows += q[kl]
    rows += c
    return rows


def stress_from_moments(x, moment):
    c2 = core_radius**2
    G = moment[0:3]
    H = [moment[3 + 3 * k : 6 + 3 * k] for k in range(3)]
    Q = [moment[12 + 3 * kl : 15 + 3 * kl] for kl in range(6)]
    C = moment[30:36]
    x2 = dot3(x, x)
    xG = dot3(x, G)
    trH = H[0][0] + H[1][1] + H[2][2]
    Z = [Q[0][n] + Q[1][n] + Q[2][n] for n in range(3)]
    W = [Q[SYM[(0, n)]][0] + Q[SYM[(1, n)]][1] + Q[SYM[(2, n)]][2] for n in range(3)]
    xH = [x[0] * H[0][n] + x[1] * H[1][n] + x[2] * H[2][n] for n in range(3)]
    Hx = [H[n][0] * x[0] + H[n][1] * x[1] + H[n][2] * x[2] for n in range(3)]
    xQ = [
        [x[0] * Q[SYM[(0, m)]][n] + x[1] * Q[SYM[(1, m)]][n] + x[2] * Q[SYM[(2, m)]][n] for n in range(3)]
        for m in range(3)
    ]
    lead = [(x2 + c2) * G[n] - 2.0 * xH[n] + Z[n] + 3.0 * Hx[n] - 3.0 * W[n] for n in range(3)]
    both = xG - trH
    diagonal = (
        (x2 + 2.5 * c2) * both
        - 2.0 * dot3(x, xH)
        + 2.0 * dot3(x, W)
        + dot3(x, Z)
    )
    out = []
    for m, n in PAIRS6:
        value = (
            x[m] * lead[n]
            + x[n] * lead[m]
            - (x2 + c2) * (H[m][n] + H[n][m])
            + 2.0 * (xQ[m][n] + xQ[n][m])
            - 3.0 * (x[m] * x[n] * both + dot3(x, Q[SYM[(m, n)]]))
            - C[SYM[(m, n)]]
        )
        if m == n:
            value = value + diagonal
        out.append(value)
    return out


PIECE_X = (0, 0, 1, 1, 0, 2)
PIECE_Y = (0, 1, 0, 1, 2, 0)


def field_rows(x):
    one = jnp.ones_like(x[0])
    rows = []
    for c in range(3):
        part = pieces(x[c], 3)
        rows += [part[j] for j in PIECE_X]
    rows += pieces(dot3(x, x) + core_radius**2, 3)
    rows += [one, one, one]
    return rows


def source_rows(y):
    one = jnp.ones_like(y[0])
    rows = []
    for c in range(3):
        part = pieces(-2.0 * y[c], 3)
        rows += [part[j] for j in PIECE_Y]
    rows += [one, one, one]
    rows += pieces(dot3(y, y), 3)
    return rows


def kernel(
    mid_any, line_any, burg_any, cell_any, node_any, glist_any, gcount_any, plist_any, pcount_any,
    nout_ref, cout_ref,
    mid, line, burg, cells_in, nodes_in, glist, gcount, plist, pcount,
    own, pkt, ghost, far, feat, FT, yrow, YT, xrow, XL, XR, R2, VH, VL, MT, mono, bl, cacc, cpkt,
    crecv, frow, nacc, npkt, nrecv, send_sem, recv_sem, load_sem,
):
    i = lax.axis_index("dx")
    j = lax.axis_index("dy")
    ndx = lax.axis_size("dx")
    ndy = lax.axis_size("dy")
    peers = [
        (lax.rem(i + (a + ndx), ndx), lax.rem(j + (b + ndy), ndy)) for a, b in neighbour_offsets
    ]

    barrier = pltpu.get_barrier_semaphore()
    for peer in peers:
        pl.semaphore_signal(barrier, inc=1, device_id=peer, device_id_type=MESH)

    def sends(kind, source, target):
        copies = []
        for k in range(8):
            copies.append(
                pltpu.make_async_remote_copy(
                    src_ref=source(k),
                    dst_ref=target.at[7 - k],
                    send_sem=send_sem.at[kind, k],
                    recv_sem=recv_sem.at[kind, 7 - k],
                    device_id=peers[k],
                    device_id_type=MESH,
                )
            )
        return copies

    loads = [
        pltpu.make_async_copy(source, target, load_sem.at[index])
        for index, (source, target) in enumerate(
            (
                (glist_any, glist),
                (gcount_any, gcount),
                (mid_any, mid),
                (line_any, line),
                (burg_any, burg),
                (plist_any, plist),
                (pcount_any, pcount),
                (cell_any, cells_in),
                (node_any, nodes_in),
            )
        )
    ]
    for load in loads:
        load.start()
    for load in loads:
        load.wait()

    own_flat = own.reshape(TILES * 16, TILE)
    for c in range(3):
        each_tile(own_flat, 16, c)[...] = mid[c]
        each_tile(own_flat, 16, 3 + c)[...] = line[c]
        each_tile(own_flat, 16, 6 + c)[...] = burg[c]
    for k in range(8):
        for g in range(GHOST):
            valid = jnp.minimum(jnp.maximum(gcount[0, 0, k] - g, 0), 1).astype(f32)
            pkt[k, :, g, :] = own[glist[g, k]][0:9] * valid

    ghost_copies = sends(0, lambda k: pkt.at[k], ghost)
    zero_rows = jnp.zeros((AUG, TILE), f32)

    def prepare_sources(first, count, y, line_rows, burgers, unroll):
        for index, value in enumerate(source_features(y, line_rows, burgers)):
            each_tile(feat, 41, index, first, count)[...] = value
        for index, value in enumerate(source_rows(y)):
            each_tile(yrow, 33, index, first, count)[...] = value
        zero = jnp.zeros_like(y[0])
        for index in range(36, FEATURES):
            each_tile(feat, 41, index, first, count)[...] = zero
        for index in range(24, AUG):
            each_tile(yrow, 33, index, first, count)[...] = zero

        def per_tile(t, carry):
            FT[t] = jnp.concatenate(pieces(tile_rows(feat, 41, t, FEATURES)[...], 3), axis=0).astype(bf16)
            rows_t = tile_rows(yrow, 33, t, AUG)[...]
            YT[0, t] = jnp.concatenate([rows_t, zero_rows], axis=0).astype(bf16).T
            YT[1, t] = jnp.concatenate([zero_rows, rows_t], axis=0).astype(bf16).T
            return carry

        lax.fori_loop(first, first + count, per_tile, 0, unroll=unroll)

    own_x = [mid[c] - 0.5 for c in range(3)]
    own_line = [line[c] for c in range(3)]
    own_burgers = [burg[c] for c in range(3)]
    prepare_sources(0, TILES, own_x, own_line, own_burgers, 8)

    field = field_rows(own_x)
    for index, value in enumerate(field):
        each_tile(xrow, 33, index)[...] = value
    for index in range(len(field), AUG):
        each_tile(xrow, 33, index)[...] = jnp.zeros((TILES, TILE), f32)

    def field_tile(t, carry):
        rows_t = tile_rows(xrow, 33, t, AUG)[...]
        XL[t] = jnp.concatenate([rows_t, zero_rows], axis=0).astype(bf16)
        XR[t] = jnp.concatenate([zero_rows, rows_t], axis=0).astype(bf16)
        return carry

    lax.fori_loop(0, TILES, field_tile, 0, unroll=8)
    FT[POOL] = jnp.zeros((3 * FEATURES, TILE), bf16)

    pl.semaphore_wait(barrier, 8)
    for copy in ghost_copies:
        copy.start()

    scaled = [2.0 * (mid[c] - 0.5) for c in range(3)]
    powers = []
    for u in scaled:
        square = u * u
        powers.append([jnp.ones_like(u), u, square, square * u, square * square])
    for r, (e0, e1, e2) in enumerate(exponent_table()):
        each_tile(mono, 41, r)[...] = powers[0][e0] * powers[1][e1] * powers[2][e2]
    for r in range(35, 40):
        each_tile(mono, 41, r)[...] = jnp.zeros((TILES, TILE), f32)
    for beta in range(3):
        for gamma in range(3):
            each_tile(bl, 9, 3 * beta + gamma)[...] = burg[beta] * line[gamma]
    cacc[...] = jnp.zeros_like(cacc)
    sub128 = lax.broadcasted_iota(jnp.int32, (TILE, TILE), 0)

    def cell_group(group, carry):
        highs, lows, members = [], [], []
        for inner in range(4):
            t = group * 4 + inner
            mono_t = tile_rows(mono, 41, t, 40)[...]
            bl_t = tile_rows(bl, 9, t, 9)[...]
            block = [bl_t[k : k + 1, :] * mono_t for k in range(9)]
            block.append(jnp.zeros((8, TILE), f32))
            terms = jnp.concatenate(block, axis=0)
            high = terms.astype(bf16)
            highs.append(high)
            lows.append((terms - high.astype(f32)).astype(bf16))
            cells = cells_in[pl.ds(t, 1), :]
            members.append(jnp.where(sub128 == cells, 1.0, 0.0).astype(bf16))
        lhs = jnp.concatenate(
            [jnp.concatenate(highs, axis=1), jnp.concatenate(lows, axis=1)], axis=0
        )
        rhs = jnp.concatenate(members, axis=1)
        cacc[...] += lax.dot_general(lhs, rhs, NT, preferred_element_type=f32)
        return carry

    lax.fori_loop(0, TILES // 4, cell_group, 0)
    for block in range(3):
        rows = min(TILE, TERMS - block * TILE)
        part = cacc[block * TILE : block * TILE + rows, :] + cacc[TERMS + block * TILE : TERMS + block * TILE + rows, :]
        if rows < TILE:
            part = jnp.concatenate([part, jnp.zeros((TILE - rows, TILE), f32)], axis=0)
        turned = part.T
        for d in range(9):
            cpkt[d, :, block * TILE : (block + 1) * TILE] = turned[8 * d : 8 * d + 8, :]
    cell_copies = sends(1, lambda k: cpkt.at[k + (k >= 4)], crecv)
    for copy in cell_copies:
        copy.start()

    for k in range(8):
        ghost_copies[k].wait()
    for q in range(8):
        a, b = neighbour_offsets[q]
        rows = pl.ds(GHOST * q, GHOST)
        far[0, rows, :] = ghost[q, 0] + float(a)
        far[1, rows, :] = ghost[q, 1] + float(b)
        for c in range(2, 9):
            far[c, rows, :] = ghost[q, c]
    prepare_sources(
        TILES,
        POOL - TILES,
        [far[c] - 0.5 for c in range(3)],
        [far[c] for c in range(3, 6)],
        [far[c] for c in range(6, 9)],
        8,
    )

    def stage_inner(t, slot):
        rhs = jnp.concatenate([XL[t], XR[t]], axis=1)
        for pair in range(NP // 2):
            lhs = YT[0, plist[2 * pair, 0, t]] + YT[1, plist[2 * pair + 1, 0, t]]
            R2[slot, pair] = jnp.dot(lhs, rhs, preferred_element_type=f32)

    def stage_power(slot):
        for n in range(NP):
            radius_sq = R2[slot, n // 2, :, (n % 2) * TILE : (n % 2 + 1) * TILE]
            inverse = lax.rsqrt(radius_sq)
            square = inverse * inverse
            value = square * square * inverse
            high = value.astype(bf16)
            VH[slot, n * TILE : (n + 1) * TILE, :] = high
            VL[slot, n * TILE : (n + 1) * TILE, :] = (value - high.astype(f32)).astype(bf16)

    def stage_sum(t, slot):
        count = pcount[0, 0, t]
        chosen = []
        for n in range(NP):
            valid = jnp.minimum(jnp.maximum(count - n, 0), 1)
            chosen.append(FT[valid * (plist[n, 0, t] - POOL) + POOL])
        weights = jnp.concatenate([VH[slot], VL[slot]], axis=1)
        total = jnp.dot(jnp.concatenate(chosen, axis=1), weights, preferred_element_type=f32)
        total = total[:, 0:TILE] + total[:, TILE : 2 * TILE]
        tile_rows(MT, 41, t, FEATURES)[...] = total[0:FEATURES] + total[FEATURES : 2 * FEATURES] + total[2 * FEATURES : 3 * FEATURES]

    stage_inner(0, 0)
    stage_power(0)
    stage_inner(1, 1)

    def pair_steps(step, carry):
        for inner in range(UNROLL):
            t = step * UNROLL + inner + 2
            stage_sum(t - 2, inner % 2)
            stage_power((inner + 1) % 2)
            stage_inner(t, inner % 2)
        return carry

    lax.fori_loop(0, (TILES - 2) // UNROLL, pair_steps, 0)
    stage_sum(TILES - 2, 0)
    stage_power(1)
    stage_sum(TILES - 1, 1)

    own_x = [mid[c] - 0.5 for c in range(3)]
    own_line = [line[c] for c in range(3)]
    own_burgers = [burg[c] for c in range(3)]
    stress = stress_from_moments(own_x, [each_tile(MT, 41, r)[...] for r in range(36)])
    traction = [dot3([stress[SYM[(m, n)]] for n in range(3)], own_burgers) for m in range(3)]
    force = cross(traction, own_line)
    for c in range(3):
        for piece, value in enumerate(pieces(0.5 * force[c], 2)):
            each_tile(frow, 9, 2 * c + piece)[...] = value
    nacc[...] = jnp.zeros_like(nacc)
    sub40 = lax.broadcasted_iota(jnp.int32, (40, TILE), 0)

    def node_group(group, carry):
        lefts, rights = [], []
        for inner in range(NODE_GROUP):
            t = group * NODE_GROUP + inner
            rows_t = tile_rows(frow, 9, t, 6)[...]
            ends = nodes_in[t]
            for end in range(2):
                nodes = ends[end : end + 1, :]
                outer = sub40 == lax.shift_right_logical(nodes, 7)
                lefts.append(
                    jnp.concatenate(
                        [jnp.where(outer, rows_t[r : r + 1, :], 0.0) for r in range(6)], axis=0
                    ).astype(bf16)
                )
                rights.append(jnp.where(sub128 == (nodes & 127), 1.0, 0.0).astype(bf16))
        nacc[...] += lax.dot_general(
            jnp.concatenate(lefts, axis=1),
            jnp.concatenate(rights, axis=1),
            NT,
            preferred_element_type=f32,
        )
        return carry

    lax.fori_loop(0, TILES // NODE_GROUP, node_group, 0)
    for c in range(3):
        total = nacc[80 * c : 80 * c + 40, :] + nacc[80 * c + 40 : 80 * c + 80, :]
        for d in range(9):
            npkt[d, c] = total[4 * d : 4 * d + 4, :]
    node_copies = sends(2, lambda k: npkt.at[k + (k >= 4)], nrecv)
    for copy in node_copies:
        copy.start()

    for copy in cell_copies:
        copy.wait()
    moments = cpkt[4]
    for q in range(8):
        moments = moments + crecv[q]
    for k in range(9):
        cout_ref[:, 35 * k : 35 * k + 35] = moments[:, 40 * k : 40 * k + 35]
    for copy in node_copies:
        copy.wait()
    nodes = npkt[4]
    for q in range(8):
        nodes = nodes + nrecv[q]
    nout_ref[...] = nodes


def on_device(
    seg_mid, seg_line, seg_burgers, seg_cell, seg_node, ghost_list, ghost_count, pair_list, pair_count
):
    shape3 = (3, TILES, TILE)
    arguments = (
        seg_mid.reshape(shape3),
        seg_line.reshape(shape3),
        seg_burgers.reshape(shape3),
        seg_cell.reshape(TILES, TILE),
        seg_node.reshape(2, TILES, TILE).transpose(1, 0, 2),
        ghost_list.reshape(8, GHOST).T,
        ghost_count,
        pair_list.transpose(3, 0, 1, 2).reshape(NP, 1, TILES),
        pair_count,
    )
    vmem = pl.BlockSpec(memory_space=pltpu.VMEM)
    anywhere = pl.BlockSpec(memory_space=pl.ANY)
    node_force, moments = pl.pallas_call(
        kernel,
        out_shape=(
            jax.ShapeDtypeStruct((3, NODE_DEV // TILE, TILE), f32),
            jax.ShapeDtypeStruct((CELL_DEV, COMPONENTS), f32),
        ),
        in_specs=[anywhere] * 9,
        out_specs=(vmem, vmem),
        scratch_shapes=[
            pltpu.VMEM(shape3, f32),
            pltpu.VMEM(shape3, f32),
            pltpu.VMEM(shape3, f32),
            pltpu.VMEM((TILES, TILE), jnp.int32),
            pltpu.VMEM((TILES, 2, TILE), jnp.int32),
            pltpu.SMEM((GHOST, 8), jnp.int32),
            pltpu.SMEM((1, 1, 8), jnp.int32),
            pltpu.SMEM((NP, 1, TILES), jnp.int32),
            pltpu.SMEM((1, 1, TILES), jnp.int32),
            pltpu.VMEM((TILES, 16, TILE), f32),
            pltpu.VMEM((8, 9, GHOST, TILE), f32),
            pltpu.VMEM((8, 9, GHOST, TILE), f32),
            pltpu.VMEM((9, POOL - TILES, TILE), f32),
            pltpu.VMEM((POOL * 41, TILE), f32),
            pltpu.VMEM((POOL + 1, 3 * FEATURES, TILE), bf16),
            pltpu.VMEM((POOL * 33, TILE), f32),
            pltpu.VMEM((2, POOL, TILE, 2 * AUG), bf16),
            pltpu.VMEM((TILES * 33, TILE), f32),
            pltpu.VMEM((TILES, 2 * AUG, TILE), bf16),
            pltpu.VMEM((TILES, 2 * AUG, TILE), bf16),
            pltpu.VMEM((2, NP // 2, TILE, 2 * TILE), f32),
            pltpu.VMEM((2, NP * TILE, TILE), bf16),
            pltpu.VMEM((2, NP * TILE, TILE), bf16),
            pltpu.VMEM((TILES * 41, TILE), f32),
            pltpu.VMEM((TILES * 41, TILE), f32),
            pltpu.VMEM((TILES * 9, TILE), f32),
            pltpu.VMEM((2 * TERMS, TILE), f32),
            pltpu.VMEM((9, CELL_DEV, 384), f32),
            pltpu.VMEM((8, CELL_DEV, 384), f32),
            pltpu.VMEM((TILES * 9, TILE), f32),
            pltpu.VMEM((240, TILE), f32),
            pltpu.VMEM((9, 3, 4, TILE), f32),
            pltpu.VMEM((8, 3, 4, TILE), f32),
            pltpu.SemaphoreType.DMA((3, 8)),
            pltpu.SemaphoreType.DMA((3, 8)),
            pltpu.SemaphoreType.DMA((9,)),
        ],
        compiler_params=pltpu.CompilerParams(
            collective_id=0, has_side_effects=True, vmem_limit_bytes=40 * 1024 * 1024
        ),
        name="segments",
    )(*[pltpu.with_memory_space_constraint(value, pltpu.HBM) for value in arguments])
    return node_force.reshape(1, 1, 3, NODE_DEV), moments.T


def solution(mesh):
    in_specs = (
        P("dx", "dy", None, None),
        P("dx", "dy", None, None),
        P("dx", "dy", None, None),
        P("dx", "dy", None),
        P("dx", "dy", None, None),
        P("dx", "dy", None, None),
        P("dx", "dy", None),
        P("dx", "dy", None, None),
        P("dx", "dy", None),
    )
    out_specs = (P("dx", "dy", None, None), P(None, ("dx", "dy")))
    return jax.shard_map(
        on_device, mesh=mesh, in_specs=in_specs, out_specs=out_specs, check_vma=False
    )
```

```python
import jax
import jax.numpy as jnp
from jax import lax
from jax.experimental import pallas as pl
from jax.experimental.pallas import tpu as pltpu
from jax.sharding import PartitionSpec as P

TILE = 128
TILES = 32
GHOST = 2
NP = 12
NODE_DEV = 512
CELL_DEV = 8
COMPONENTS = 315
POOL = 48
FEATURES = 40
AUG = 32
UNROLL = 30
NODE_GROUP = 16
NODE_ROWS = 216
TERMS = 368

core_radius = 0.1
shear_scale = 0.25
neighbour_offsets = ((-1, -1), (-1, 0), (-1, 1), (0, -1), (0, 1), (1, -1), (1, 0), (1, 1))
f32 = jnp.float32
bf16 = jnp.bfloat16
MESH = pl.DeviceIdType.MESH
SEND_ORDER = (0, 2, 5, 7, 1, 6, 3, 4)
NT = (((1,), (1,)), ((), ()))


def rounded(value):
    return value.astype(bf16).astype(f32)


def pieces(value, count):
    parts = []
    for _ in range(count - 1):
        part = rounded(value)
        parts.append(part)
        value = value - part
    parts.append(rounded(value))
    return parts


def each_tile(ref, pitch, index, first=0, count=TILES):
    return ref.at[pl.ds(first * pitch + index, count, stride=pitch), :]


def tile_rows(ref, pitch, t, rows):
    return ref.at[pl.ds(t * pitch, rows), :]


def exponent_table():
    exponent_rows = []
    for degree in range(5):
        for first_power in range(degree, -1, -1):
            for second in range(degree - first_power, -1, -1):
                exponent_rows.append((first_power, second, degree - first_power - second))
    return exponent_rows


def cross(u, v):
    return [
        u[1] * v[2] - u[2] * v[1],
        u[2] * v[0] - u[0] * v[2],
        u[0] * v[1] - u[1] * v[0],
    ]


def dot3(u, v):
    return u[0] * v[0] + u[1] * v[1] + u[2] * v[2]


PAIRS6 = ((0, 0), (1, 1), (2, 2), (0, 1), (0, 2), (1, 2))
SYM = {}
for _slot, (_m, _n) in enumerate(PAIRS6):
    SYM[(_m, _n)] = _slot
    SYM[(_n, _m)] = _slot


def source_features(y, line, burgers):
    g = [shear_scale * v for v in cross(burgers, line)]
    h = [[y[k] * g[n] for n in range(3)] for k in range(3)]
    q = [[y[k] * h[l][n] for n in range(3)] for (k, l) in PAIRS6]
    y2 = dot3(y, y)
    trace = h[0][0] + h[1][1] + h[2][2]
    c = []
    for m, n in PAIRS6:
        value = y2 * (h[m][n] + h[n][m]) - 3.0 * trace * (y[m] * y[n])
        if m == n:
            value = value + y2 * trace
        c.append(value)
    rows = list(g)
    for k in range(3):
        rows += h[k]
    for kl in range(6):
        rows += q[kl]
    rows += c
    return rows


def stress_from_moments(x, moment):
    c2 = core_radius**2
    G = moment[0:3]
    H = [moment[3 + 3 * k : 6 + 3 * k] for k in range(3)]
    Q = [moment[12 + 3 * kl : 15 + 3 * kl] for kl in range(6)]
    C = moment[30:36]
    x2 = dot3(x, x)
    xG = dot3(x, G)
    trH = H[0][0] + H[1][1] + H[2][2]
    Z = [Q[0][n] + Q[1][n] + Q[2][n] for n in range(3)]
    W = [Q[SYM[(0, n)]][0] + Q[SYM[(1, n)]][1] + Q[SYM[(2, n)]][2] for n in range(3)]
    xH = [x[0] * H[0][n] + x[1] * H[1][n] + x[2] * H[2][n] for n in range(3)]
    Hx = [H[n][0] * x[0] + H[n][1] * x[1] + H[n][2] * x[2] for n in range(3)]
    xQ = [
        [x[0] * Q[SYM[(0, m)]][n] + x[1] * Q[SYM[(1, m)]][n] + x[2] * Q[SYM[(2, m)]][n] for n in range(3)]
        for m in range(3)
    ]
    lead = [(x2 + c2) * G[n] - 2.0 * xH[n] + Z[n] + 3.0 * Hx[n] - 3.0 * W[n] for n in range(3)]
    both = xG - trH
    diagonal = (
        (x2 + 2.5 * c2) * both
        - 2.0 * dot3(x, xH)
        + 2.0 * dot3(x, W)
        + dot3(x, Z)
    )
    out = []
    for m, n in PAIRS6:
        value = (
            x[m] * lead[n]
            + x[n] * lead[m]
            - (x2 + c2) * (H[m][n] + H[n][m])
            + 2.0 * (xQ[m][n] + xQ[n][m])
            - 3.0 * (x[m] * x[n] * both + dot3(x, Q[SYM[(m, n)]]))
            - C[SYM[(m, n)]]
        )
        if m == n:
            value = value + diagonal
        out.append(value)
    return out


PIECE_X = (0, 0, 1, 1, 0, 2)
PIECE_Y = (0, 1, 0, 1, 2, 0)


def field_rows(x):
    one = jnp.ones_like(x[0])
    rows = []
    for c in range(3):
        part = pieces(x[c], 3)
        rows += [part[j] for j in PIECE_X]
    rows += pieces(dot3(x, x) + core_radius**2, 3)
    rows += [one, one, one]
    return rows


def source_rows(y):
    one = jnp.ones_like(y[0])
    rows = []
    for c in range(3):
        part = pieces(-2.0 * y[c], 3)
        rows += [part[j] for j in PIECE_Y]
    rows += [one, one, one]
    rows += pieces(dot3(y, y), 3)
    return rows


def kernel(
    mid_any, line_any, burg_any, cell_any, node_any, glist_any, gcount_any, plist_any, pcount_any,
    nout_ref, cout_ref,
    mid, line, burg, cells_in, nodes_in, glist, gcount, plist, pcount,
    own, pkt, ghost, far, feat, FT, yrow, YT, xrow, XL, XR, R2, VH, VL, MT, mono, bl, cacc, cpkt,
    crecv, frow, nacc, npkt, nrecv, send_sem, recv_sem, load_sem,
):
    i = lax.axis_index("dx")
    j = lax.axis_index("dy")
    ndx = lax.axis_size("dx")
    ndy = lax.axis_size("dy")
    peers = [
        (lax.rem(i + (a + ndx), ndx), lax.rem(j + (b + ndy), ndy)) for a, b in neighbour_offsets
    ]

    barrier = pltpu.get_barrier_semaphore()
    for peer in peers:
        pl.semaphore_signal(barrier, inc=1, device_id=peer, device_id_type=MESH)

    def sends(kind, source, target):
        copies = []
        for k in range(8):
            copies.append(
                pltpu.make_async_remote_copy(
                    src_ref=source(k),
                    dst_ref=target.at[7 - k],
                    send_sem=send_sem.at[kind, k],
                    recv_sem=recv_sem.at[kind, 7 - k],
                    device_id=peers[k],
                    device_id_type=MESH,
                )
            )
        return copies

    loads = [
        pltpu.make_async_copy(source, target, load_sem.at[index])
        for index, (source, target) in enumerate(
            (
                (glist_any, glist),
                (gcount_any, gcount),
                (mid_any, mid),
                (line_any, line),
                (burg_any, burg),
                (plist_any, plist),
                (pcount_any, pcount),
                (cell_any, cells_in),
                (node_any, nodes_in),
            )
        )
    ]
    for load in loads:
        load.start()
    for load in loads:
        load.wait()

    own_flat = own.reshape(TILES * 16, TILE)
    for c in range(3):
        each_tile(own_flat, 16, c)[...] = mid[c]
        each_tile(own_flat, 16, 3 + c)[...] = line[c]
        each_tile(own_flat, 16, 6 + c)[...] = burg[c]
    for k in range(8):
        for g in range(GHOST):
            valid = jnp.minimum(jnp.maximum(gcount[0, 0, k] - g, 0), 1).astype(f32)
            pkt[k, :, g, :] = own[glist[g, k]][0:9] * valid

    ghost_copies = sends(0, lambda k: pkt.at[k], ghost)
    zero_rows = jnp.zeros((AUG, TILE), f32)

    def prepare_sources(first, count, y, line_rows, burgers, unroll):
        for index, value in enumerate(source_features(y, line_rows, burgers)):
            each_tile(feat, 41, index, first, count)[...] = value
        for index, value in enumerate(source_rows(y)):
            each_tile(yrow, 33, index, first, count)[...] = value
        zero = jnp.zeros_like(y[0])
        for index in range(36, FEATURES):
            each_tile(feat, 41, index, first, count)[...] = zero
        for index in range(24, AUG):
            each_tile(yrow, 33, index, first, count)[...] = zero

        def per_tile(t, carry):
            FT[t] = jnp.concatenate(pieces(tile_rows(feat, 41, t, FEATURES)[...], 3), axis=0).astype(bf16)
            rows_t = tile_rows(yrow, 33, t, AUG)[...]
            YT[0, t] = jnp.concatenate([rows_t, zero_rows], axis=0).astype(bf16).T
            YT[1, t] = jnp.concatenate([zero_rows, rows_t], axis=0).astype(bf16).T
            return carry

        lax.fori_loop(first, first + count, per_tile, 0, unroll=unroll)

    own_x = [mid[c] - 0.5 for c in range(3)]
    own_line = [line[c] for c in range(3)]
    own_burgers = [burg[c] for c in range(3)]
    prepare_sources(0, TILES, own_x, own_line, own_burgers, 8)

    field = field_rows(own_x)
    for index, value in enumerate(field):
        each_tile(xrow, 33, index)[...] = value
    for index in range(len(field), AUG):
        each_tile(xrow, 33, index)[...] = jnp.zeros((TILES, TILE), f32)

    def field_tile(t, carry):
        rows_t = tile_rows(xrow, 33, t, AUG)[...]
        XL[t] = jnp.concatenate([rows_t, zero_rows], axis=0).astype(bf16)
        XR[t] = jnp.concatenate([zero_rows, rows_t], axis=0).astype(bf16)
        return carry

    lax.fori_loop(0, TILES, field_tile, 0, unroll=8)
    FT[POOL] = jnp.zeros((3 * FEATURES, TILE), bf16)

    pl.semaphore_wait(barrier, 8)
    for k in SEND_ORDER:
        ghost_copies[k].start()

    scaled = [2.0 * (mid[c] - 0.5) for c in range(3)]
    powers = []
    for u in scaled:
        square = u * u
        powers.append([jnp.ones_like(u), u, square, square * u, square * square])
    for r, (e0, e1, e2) in enumerate(exponent_table()):
        each_tile(mono, 41, r)[...] = powers[0][e0] * powers[1][e1] * powers[2][e2]
    for r in range(35, 40):
        each_tile(mono, 41, r)[...] = jnp.zeros((TILES, TILE), f32)
    for beta in range(3):
        for gamma in range(3):
            each_tile(bl, 9, 3 * beta + gamma)[...] = burg[beta] * line[gamma]
    cacc[...] = jnp.zeros_like(cacc)
    sub128 = lax.broadcasted_iota(jnp.int32, (TILE, TILE), 0)

    def cell_group(group, carry):
        highs, lows, members = [], [], []
        for inner in range(4):
            t = group * 4 + inner
            mono_t = tile_rows(mono, 41, t, 40)[...]
            bl_t = tile_rows(bl, 9, t, 9)[...]
            block = [bl_t[k : k + 1, :] * mono_t for k in range(9)]
            block.append(jnp.zeros((8, TILE), f32))
            terms = jnp.concatenate(block, axis=0)
            high = terms.astype(bf16)
            highs.append(high)
            lows.append((terms - high.astype(f32)).astype(bf16))
            cells = cells_in[pl.ds(t, 1), :]
            members.append(jnp.where(sub128 == cells, 1.0, 0.0).astype(bf16))
        lhs = jnp.concatenate(
            [jnp.concatenate(highs, axis=1), jnp.concatenate(lows, axis=1)], axis=0
        )
        rhs = jnp.concatenate(members, axis=1)
        cacc[...] += lax.dot_general(lhs, rhs, NT, preferred_element_type=f32)
        return carry

    lax.fori_loop(0, TILES // 4, cell_group, 0)
    for block in range(3):
        rows = min(TILE, TERMS - block * TILE)
        part = cacc[block * TILE : block * TILE + rows, :] + cacc[TERMS + block * TILE : TERMS + block * TILE + rows, :]
        if rows < TILE:
            part = jnp.concatenate([part, jnp.zeros((TILE - rows, TILE), f32)], axis=0)
        turned = part.T
        for d in range(9):
            cpkt[d, :, block * TILE : (block + 1) * TILE] = turned[8 * d : 8 * d + 8, :]
    cell_copies = sends(1, lambda k: cpkt.at[k + (k >= 4)], crecv)
    for k in SEND_ORDER:
        cell_copies[k].start()

    for k in range(8):
        ghost_copies[k].wait()
    for q in range(8):
        a, b = neighbour_offsets[q]
        rows = pl.ds(GHOST * q, GHOST)
        far[0, rows, :] = ghost[q, 0] + float(a)
        far[1, rows, :] = ghost[q, 1] + float(b)
        for c in range(2, 9):
            far[c, rows, :] = ghost[q, c]
    prepare_sources(
        TILES,
        POOL - TILES,
        [far[c] - 0.5 for c in range(3)],
        [far[c] for c in range(3, 6)],
        [far[c] for c in range(6, 9)],
        16,
    )

    def stage_inner(t, slot):
        rhs = jnp.concatenate([XL[t], XR[t]], axis=1)
        for pair in range(NP // 2):
            lhs = YT[0, plist[2 * pair, 0, t]] + YT[1, plist[2 * pair + 1, 0, t]]
            R2[slot, pair] = jnp.dot(lhs, rhs, preferred_element_type=f32)

    def stage_power(slot):
        for n in range(NP):
            radius_sq = R2[slot, n // 2, :, (n % 2) * TILE : (n % 2 + 1) * TILE]
            inverse = lax.rsqrt(radius_sq)
            square = inverse * inverse
            value = square * square * inverse
            high = value.astype(bf16)
            VH[slot, n * TILE : (n + 1) * TILE, :] = high
            VL[slot, n * TILE : (n + 1) * TILE, :] = (value - high.astype(f32)).astype(bf16)

    def stage_sum(t, slot):
        count = pcount[0, 0, t]
        chosen = []
        for n in range(NP):
            valid = jnp.minimum(jnp.maximum(count - n, 0), 1)
            chosen.append(FT[valid * (plist[n, 0, t] - POOL) + POOL])
        weights = jnp.concatenate([VH[slot], VL[slot]], axis=1)
        total = jnp.dot(jnp.concatenate(chosen, axis=1), weights, preferred_element_type=f32)
        total = total[:, 0:TILE] + total[:, TILE : 2 * TILE]
        tile_rows(MT, 41, t, FEATURES)[...] = total[0:FEATURES] + total[FEATURES : 2 * FEATURES] + total[2 * FEATURES : 3 * FEATURES]

    stage_inner(0, 0)
    stage_power(0)
    stage_inner(1, 1)

    def pair_steps(step, carry):
        for inner in range(UNROLL):
            t = step * UNROLL + inner + 2
            stage_sum(t - 2, inner % 2)
            stage_power((inner + 1) % 2)
            stage_inner(t, inner % 2)
        return carry

    lax.fori_loop(0, (TILES - 2) // UNROLL, pair_steps, 0)
    stage_sum(TILES - 2, 0)
    stage_power(1)
    stage_sum(TILES - 1, 1)

    own_x = [mid[c] - 0.5 for c in range(3)]
    own_line = [line[c] for c in range(3)]
    own_burgers = [burg[c] for c in range(3)]
    stress = stress_from_moments(own_x, [each_tile(MT, 41, r)[...] for r in range(36)])
    traction = [dot3([stress[SYM[(m, n)]] for n in range(3)], own_burgers) for m in range(3)]
    force = cross(traction, own_line)
    for c in range(3):
        for piece, value in enumerate(pieces(0.5 * force[c], 2)):
            for copy_index in range(4):
                each_tile(frow, 25, 6 * copy_index + 2 * c + piece)[...] = value
    nacc[...] = jnp.zeros_like(nacc)
    row_node = lax.broadcasted_iota(jnp.int32, (NODE_ROWS, TILE), 0) // 6

    def node_group(group, carry):
        lefts, rights = [], []
        for inner in range(NODE_GROUP):
            t = group * NODE_GROUP + inner
            rows_t = tile_rows(frow, 25, t, 24)[...]
            rows_t = jnp.concatenate([rows_t] * 9, axis=0)
            ends = nodes_in[t]
            for end in range(2):
                nodes = ends[end : end + 1, :]
                outer = row_node == lax.shift_right_logical(nodes, 7)
                lefts.append(jnp.where(outer, rows_t, 0.0).astype(bf16))
                rights.append(jnp.where(sub128 == (nodes & 127), 1.0, 0.0).astype(bf16))
        nacc[...] += lax.dot_general(
            jnp.concatenate(lefts, axis=1),
            jnp.concatenate(rights, axis=1),
            NT,
            preferred_element_type=f32,
        )
        return carry

    lax.fori_loop(0, TILES // NODE_GROUP, node_group, 0)
    for d in range(9):
        for c in range(3):
            first = 24 * d + 2 * c
            npkt[d, c] = nacc[pl.ds(first, 4, stride=6), :] + nacc[pl.ds(first + 1, 4, stride=6), :]
    node_copies = sends(2, lambda k: npkt.at[k + (k >= 4)], nrecv)
    for k in SEND_ORDER:
        node_copies[k].start()

    for copy in cell_copies:
        copy.wait()
    moments = cpkt[4]
    for q in range(8):
        moments = moments + crecv[q]
    for k in range(9):
        cout_ref[:, 35 * k : 35 * k + 35] = moments[:, 40 * k : 40 * k + 35]
    for copy in node_copies:
        copy.wait()
    nodes = npkt[4]
    for q in range(8):
        nodes = nodes + nrecv[q]
    nout_ref[...] = nodes


def hand_over(node_in, moments_in, node_out, moments_out):
    node_out[...] = node_in[...]
    moments_out[...] = moments_in[...]


def on_device(
    seg_mid, seg_line, seg_burgers, seg_cell, seg_node, ghost_list, ghost_count, pair_list, pair_count
):
    shape3 = (3, TILES, TILE)
    arguments = (
        seg_mid.reshape(shape3),
        seg_line.reshape(shape3),
        seg_burgers.reshape(shape3),
        seg_cell.reshape(TILES, TILE),
        seg_node.reshape(2, TILES, TILE).transpose(1, 0, 2),
        ghost_list.reshape(8, GHOST).T,
        ghost_count,
        pair_list.transpose(3, 0, 1, 2).reshape(NP, 1, TILES),
        pair_count,
    )
    vmem = pl.BlockSpec(memory_space=pltpu.VMEM)
    anywhere = pl.BlockSpec(memory_space=pl.ANY)
    node_force, moments = pl.pallas_call(
        kernel,
        out_shape=(
            jax.ShapeDtypeStruct((3, NODE_DEV // TILE, TILE), f32),
            jax.ShapeDtypeStruct((CELL_DEV, COMPONENTS), f32),
        ),
        in_specs=[anywhere] * 9,
        out_specs=(vmem, vmem),
        scratch_shapes=[
            pltpu.VMEM(shape3, f32),
            pltpu.VMEM(shape3, f32),
            pltpu.VMEM(shape3, f32),
            pltpu.VMEM((TILES, TILE), jnp.int32),
            pltpu.VMEM((TILES, 2, TILE), jnp.int32),
            pltpu.SMEM((GHOST, 8), jnp.int32),
            pltpu.SMEM((1, 1, 8), jnp.int32),
            pltpu.SMEM((NP, 1, TILES), jnp.int32),
            pltpu.SMEM((1, 1, TILES), jnp.int32),
            pltpu.VMEM((TILES, 16, TILE), f32),
            pltpu.VMEM((8, 9, GHOST, TILE), f32),
            pltpu.VMEM((8, 9, GHOST, TILE), f32),
            pltpu.VMEM((9, POOL - TILES, TILE), f32),
            pltpu.VMEM((POOL * 41, TILE), f32),
            pltpu.VMEM((POOL + 1, 3 * FEATURES, TILE), bf16),
            pltpu.VMEM((POOL * 33, TILE), f32),
            pltpu.VMEM((2, POOL, TILE, 2 * AUG), bf16),
            pltpu.VMEM((TILES * 33, TILE), f32),
            pltpu.VMEM((TILES, 2 * AUG, TILE), bf16),
            pltpu.VMEM((TILES, 2 * AUG, TILE), bf16),
            pltpu.VMEM((2, NP // 2, TILE, 2 * TILE), f32),
            pltpu.VMEM((2, NP * TILE, TILE), bf16),
            pltpu.VMEM((2, NP * TILE, TILE), bf16),
            pltpu.VMEM((TILES * 41, TILE), f32),
            pltpu.VMEM((TILES * 41, TILE), f32),
            pltpu.VMEM((TILES * 9, TILE), f32),
            pltpu.VMEM((2 * TERMS, TILE), f32),
            pltpu.VMEM((9, CELL_DEV, 384), f32),
            pltpu.VMEM((8, CELL_DEV, 384), f32),
            pltpu.VMEM((TILES * 25, TILE), f32),
            pltpu.VMEM((NODE_ROWS, TILE), f32),
            pltpu.VMEM((9, 3, 4, TILE), f32),
            pltpu.VMEM((8, 3, 4, TILE), f32),
            pltpu.SemaphoreType.DMA((3, 8)),
            pltpu.SemaphoreType.DMA((3, 8)),
            pltpu.SemaphoreType.DMA((9,)),
        ],
        compiler_params=pltpu.CompilerParams(
            collective_id=0, has_side_effects=True, vmem_limit_bytes=40 * 1024 * 1024
        ),
        name="segments",
    )(*[pltpu.with_memory_space_constraint(value, pltpu.HBM) for value in arguments])
    node_force, moments = pl.pallas_call(
        hand_over,
        out_shape=(
            jax.ShapeDtypeStruct(node_force.shape, f32),
            jax.ShapeDtypeStruct(moments.shape, f32),
        ),
        in_specs=[vmem, vmem],
        out_specs=(vmem, vmem),
        compiler_params=pltpu.CompilerParams(vmem_limit_bytes=1024 * 1024),
        name="outputs",
    )(node_force, moments)
    return node_force.reshape(1, 1, 3, NODE_DEV), moments.T


def solution(mesh):
    in_specs = (
        P("dx", "dy", None, None),
        P("dx", "dy", None, None),
        P("dx", "dy", None, None),
        P("dx", "dy", None),
        P("dx", "dy", None, None),
        P("dx", "dy", None, None),
        P("dx", "dy", None),
        P("dx", "dy", None, None),
        P("dx", "dy", None),
    )
    out_specs = (P("dx", "dy", None, None), P(None, ("dx", "dy")))
    return jax.shard_map(
        on_device, mesh=mesh, in_specs=in_specs, out_specs=out_specs, check_vma=False
    )
```

```python
import jax
import jax.numpy as jnp
from jax import lax
from jax.experimental import pallas as pl
from jax.experimental.pallas import tpu as pltpu
from jax.sharding import PartitionSpec as P

TILE = 128
TILES = 32
GHOST = 2
NP = 12
NODE_DEV = 512
CELL_DEV = 8
COMPONENTS = 315
POOL = 48
FEATURES = 40
SUM_ROWS = 112
AUG = 32
UNROLL = 30
NODE_GROUP = 32
NODE_ROWS = 216
TERMS = 368

core_radius = 0.1
shear_scale = 0.25
neighbour_offsets = ((-1, -1), (-1, 0), (-1, 1), (0, -1), (0, 1), (1, -1), (1, 0), (1, 1))
f32 = jnp.float32
bf16 = jnp.bfloat16
MESH = pl.DeviceIdType.MESH
SEND_ORDER = (0, 2, 5, 7, 1, 6, 3, 4)
NT = (((1,), (1,)), ((), ()))


def rounded(value):
    return value.astype(bf16).astype(f32)


def pieces(value, count):
    parts = []
    for _ in range(count - 1):
        part = rounded(value)
        parts.append(part)
        value = value - part
    parts.append(rounded(value))
    return parts


def each_tile(ref, pitch, index, first=0, count=TILES):
    return ref.at[pl.ds(first * pitch + index, count, stride=pitch), :]


def tile_rows(ref, pitch, t, rows):
    return ref.at[pl.ds(t * pitch, rows), :]


def exponent_table():
    exponent_rows = []
    for degree in range(5):
        for first_power in range(degree, -1, -1):
            for second in range(degree - first_power, -1, -1):
                exponent_rows.append((first_power, second, degree - first_power - second))
    return exponent_rows


def cross(u, v):
    return [
        u[1] * v[2] - u[2] * v[1],
        u[2] * v[0] - u[0] * v[2],
        u[0] * v[1] - u[1] * v[0],
    ]


def dot3(u, v):
    return u[0] * v[0] + u[1] * v[1] + u[2] * v[2]


PAIRS6 = ((0, 0), (1, 1), (2, 2), (0, 1), (0, 2), (1, 2))
SYM = {}
for _slot, (_m, _n) in enumerate(PAIRS6):
    SYM[(_m, _n)] = _slot
    SYM[(_n, _m)] = _slot


def source_features(y, line, burgers):
    g = [shear_scale * v for v in cross(burgers, line)]
    h = [[y[k] * g[n] for n in range(3)] for k in range(3)]
    q = [[y[k] * h[l][n] for n in range(3)] for (k, l) in PAIRS6]
    y2 = dot3(y, y)
    trace = h[0][0] + h[1][1] + h[2][2]
    c = []
    for m, n in PAIRS6:
        value = y2 * (h[m][n] + h[n][m]) - 3.0 * trace * (y[m] * y[n])
        if m == n:
            value = value + y2 * trace
        c.append(value)
    rows = list(g)
    for k in range(3):
        rows += h[k]
    for kl in range(6):
        rows += q[kl]
    rows += c
    return rows


def stress_from_moments(x, moment):
    c2 = core_radius**2
    G = moment[0:3]
    H = [moment[3 + 3 * k : 6 + 3 * k] for k in range(3)]
    Q = [moment[12 + 3 * kl : 15 + 3 * kl] for kl in range(6)]
    C = moment[30:36]
    x2 = dot3(x, x)
    xG = dot3(x, G)
    trH = H[0][0] + H[1][1] + H[2][2]
    Z = [Q[0][n] + Q[1][n] + Q[2][n] for n in range(3)]
    W = [Q[SYM[(0, n)]][0] + Q[SYM[(1, n)]][1] + Q[SYM[(2, n)]][2] for n in range(3)]
    xH = [x[0] * H[0][n] + x[1] * H[1][n] + x[2] * H[2][n] for n in range(3)]
    Hx = [H[n][0] * x[0] + H[n][1] * x[1] + H[n][2] * x[2] for n in range(3)]
    xQ = [
        [x[0] * Q[SYM[(0, m)]][n] + x[1] * Q[SYM[(1, m)]][n] + x[2] * Q[SYM[(2, m)]][n] for n in range(3)]
        for m in range(3)
    ]
    lead = [(x2 + c2) * G[n] - 2.0 * xH[n] + Z[n] + 3.0 * Hx[n] - 3.0 * W[n] for n in range(3)]
    both = xG - trH
    diagonal = (
        (x2 + 2.5 * c2) * both
        - 2.0 * dot3(x, xH)
        + 2.0 * dot3(x, W)
        + dot3(x, Z)
    )
    out = []
    for m, n in PAIRS6:
        value = (
            x[m] * lead[n]
            + x[n] * lead[m]
            - (x2 + c2) * (H[m][n] + H[n][m])
            + 2.0 * (xQ[m][n] + xQ[n][m])
            - 3.0 * (x[m] * x[n] * both + dot3(x, Q[SYM[(m, n)]]))
            - C[SYM[(m, n)]]
        )
        if m == n:
            value = value + diagonal
        out.append(value)
    return out


PIECE_X = (0, 0, 1, 1, 0, 2)
PIECE_Y = (0, 1, 0, 1, 2, 0)


def field_rows(x):
    one = jnp.ones_like(x[0])
    rows = []
    for c in range(3):
        part = pieces(x[c], 3)
        rows += [part[j] for j in PIECE_X]
    rows += pieces(dot3(x, x) + core_radius**2, 3)
    rows += [one, one, one]
    return rows


def source_rows(y):
    one = jnp.ones_like(y[0])
    rows = []
    for c in range(3):
        part = pieces(-2.0 * y[c], 3)
        rows += [part[j] for j in PIECE_Y]
    rows += [one, one, one]
    rows += pieces(dot3(y, y), 3)
    return rows


def kernel(
    mid_any, line_any, burg_any, cell_any, node_any, glist_any, gcount_any, plist_any, pcount_any,
    nout_ref, cout_ref,
    mid, line, burg, cells_in, nodes_in, glist, gcount, plist, pcount,
    own, pkt, ghost, far, feat, FT, yrow, YT, xrow, XL, XR, VH, VL, MT, mono, bl, cacc, cpkt,
    crecv, frow, nacc, npkt, nrecv, send_sem, recv_sem, load_sem,
):
    i = lax.axis_index("dx")
    j = lax.axis_index("dy")
    ndx = lax.axis_size("dx")
    ndy = lax.axis_size("dy")
    peers = [
        (lax.rem(i + (a + ndx), ndx), lax.rem(j + (b + ndy), ndy)) for a, b in neighbour_offsets
    ]

    barrier = pltpu.get_barrier_semaphore()
    for peer in peers:
        pl.semaphore_signal(barrier, inc=1, device_id=peer, device_id_type=MESH)

    def sends(kind, source, target):
        copies = []
        for k in range(8):
            copies.append(
                pltpu.make_async_remote_copy(
                    src_ref=source(k),
                    dst_ref=target.at[7 - k],
                    send_sem=send_sem.at[kind, k],
                    recv_sem=recv_sem.at[kind, 7 - k],
                    device_id=peers[k],
                    device_id_type=MESH,
                )
            )
        return copies

    loads = [
        pltpu.make_async_copy(source, target, load_sem.at[index])
        for index, (source, target) in enumerate(
            (
                (glist_any, glist),
                (gcount_any, gcount),
                (mid_any, mid),
                (line_any, line),
                (burg_any, burg),
                (plist_any, plist),
                (pcount_any, pcount),
                (cell_any, cells_in),
                (node_any, nodes_in),
            )
        )
    ]
    for load in loads:
        load.start()
    for load in loads:
        load.wait()

    own_flat = own.reshape(TILES * 16, TILE)
    for c in range(3):
        each_tile(own_flat, 16, c)[...] = mid[c]
        each_tile(own_flat, 16, 3 + c)[...] = line[c]
        each_tile(own_flat, 16, 6 + c)[...] = burg[c]
    for k in range(8):
        for g in range(GHOST):
            valid = jnp.minimum(jnp.maximum(gcount[0, 0, k] - g, 0), 1).astype(f32)
            pkt[k, :, g, :] = own[glist[g, k]][0:9] * valid

    ghost_copies = sends(0, lambda k: pkt.at[k], ghost)
    zero_rows = jnp.zeros((AUG, TILE), f32)

    def prepare_sources(first, count, y, line_rows, burgers, unroll):
        for index, value in enumerate(source_features(y, line_rows, burgers)):
            each_tile(feat, 41, index, first, count)[...] = value
        for index, value in enumerate(source_rows(y)):
            each_tile(yrow, 33, index, first, count)[...] = value
        zero = jnp.zeros_like(y[0])
        for index in range(36, FEATURES):
            each_tile(feat, 41, index, first, count)[...] = zero
        for index in range(24, AUG):
            each_tile(yrow, 33, index, first, count)[...] = zero

        def per_tile(t, carry):
            parts = pieces(tile_rows(feat, 41, t, FEATURES)[...], 3)
            parts = [part[0:32] for part in parts] + [part[32:36] for part in parts]
            FT[t] = jnp.concatenate(parts + [zero_rows[0:4]], axis=0).astype(bf16)
            rows_t = tile_rows(yrow, 33, t, AUG)[...]
            YT[t] = jnp.concatenate([rows_t, rows_t, zero_rows, zero_rows], axis=0).astype(bf16).T
            return carry

        lax.fori_loop(first, first + count, per_tile, 0, unroll=unroll)

    own_x = [mid[c] - 0.5 for c in range(3)]
    own_line = [line[c] for c in range(3)]
    own_burgers = [burg[c] for c in range(3)]
    prepare_sources(0, TILES, own_x, own_line, own_burgers, 8)

    field = field_rows(own_x)
    for index, value in enumerate(field):
        each_tile(xrow, 33, index)[...] = value
    for index in range(len(field), AUG):
        each_tile(xrow, 33, index)[...] = jnp.zeros((TILES, TILE), f32)

    def field_tile(t, carry):
        rows_t = tile_rows(xrow, 33, t, AUG)[...]
        XL[t] = jnp.concatenate([rows_t, zero_rows], axis=0).astype(bf16)
        XR[t] = jnp.concatenate([zero_rows, rows_t], axis=0).astype(bf16)
        return carry

    lax.fori_loop(0, TILES, field_tile, 0, unroll=8)
    FT[POOL] = jnp.zeros((SUM_ROWS, TILE), bf16)

    pl.semaphore_wait(barrier, 8)
    for k in SEND_ORDER:
        ghost_copies[k].start()

    scaled = [2.0 * (mid[c] - 0.5) for c in range(3)]
    powers = []
    for u in scaled:
        square = u * u
        powers.append([jnp.ones_like(u), u, square, square * u, square * square])
    for r, (e0, e1, e2) in enumerate(exponent_table()):
        each_tile(mono, 41, r)[...] = powers[0][e0] * powers[1][e1] * powers[2][e2]
    for r in range(35, 40):
        each_tile(mono, 41, r)[...] = jnp.zeros((TILES, TILE), f32)
    for beta in range(3):
        for gamma in range(3):
            each_tile(bl, 9, 3 * beta + gamma)[...] = burg[beta] * line[gamma]
    cacc[...] = jnp.zeros_like(cacc)
    sub128 = lax.broadcasted_iota(jnp.int32, (TILE, TILE), 0)

    def cell_group(group, carry):
        highs, lows, members = [], [], []
        for inner in range(4):
            t = group * 4 + inner
            mono_t = tile_rows(mono, 41, t, 40)[...]
            bl_t = tile_rows(bl, 9, t, 9)[...]
            block = [bl_t[k : k + 1, :] * mono_t for k in range(9)]
            block.append(jnp.zeros((8, TILE), f32))
            terms = jnp.concatenate(block, axis=0)
            high = terms.astype(bf16)
            highs.append(high)
            lows.append((terms - high.astype(f32)).astype(bf16))
            cells = cells_in[pl.ds(t, 1), :]
            members.append(jnp.where(sub128 == cells, 1.0, 0.0).astype(bf16))
        lhs = jnp.concatenate(
            [jnp.concatenate(highs, axis=1), jnp.concatenate(lows, axis=1)], axis=0
        )
        rhs = jnp.concatenate(members, axis=1)
        cacc[...] += lax.dot_general(lhs, rhs, NT, preferred_element_type=f32)
        return carry

    lax.fori_loop(0, TILES // 4, cell_group, 0)
    for block in range(3):
        rows = min(TILE, TERMS - block * TILE)
        part = cacc[block * TILE : block * TILE + rows, :] + cacc[TERMS + block * TILE : TERMS + block * TILE + rows, :]
        if rows < TILE:
            part = jnp.concatenate([part, jnp.zeros((TILE - rows, TILE), f32)], axis=0)
        turned = part.T
        for d in range(9):
            cpkt[d, :, block * TILE : (block + 1) * TILE] = turned[8 * d : 8 * d + 8, :]
    cell_copies = sends(1, lambda k: cpkt.at[k + (k >= 4)], crecv)
    for k in SEND_ORDER:
        cell_copies[k].start()

    for k in range(8):
        ghost_copies[k].wait()
    for q in range(8):
        a, b = neighbour_offsets[q]
        rows = pl.ds(GHOST * q, GHOST)
        far[0, rows, :] = ghost[q, 0] + float(a)
        far[1, rows, :] = ghost[q, 1] + float(b)
        for c in range(2, 9):
            far[c, rows, :] = ghost[q, c]
    prepare_sources(
        TILES,
        POOL - TILES,
        [far[c] - 0.5 for c in range(3)],
        [far[c] for c in range(3, 6)],
        [far[c] for c in range(6, 9)],
        16,
    )

    first_half = lax.broadcasted_iota(jnp.int32, (TILE, TILE), 1) < AUG

    def stage_power(t, slot):
        rhs = jnp.concatenate([XL[t], XR[t]], axis=1)
        for pair in range(NP // 2):
            lhs = jnp.where(first_half, YT[plist[2 * pair, 0, t]], YT[plist[2 * pair + 1, 0, t]])
            both = jnp.dot(lhs[:, 0 : 2 * AUG], rhs, preferred_element_type=f32)
            for side in range(2):
                inverse = lax.rsqrt(both[:, side * TILE : (side + 1) * TILE])
                square = inverse * inverse
                value = square * square * inverse
                high = value.astype(bf16)
                first = (2 * pair + side) * TILE
                VH[slot, first : first + TILE, :] = high
                VL[slot, first : first + TILE, :] = (value - high.astype(f32)).astype(bf16)

    def stage_sum(t, slot):
        count = pcount[0, 0, t]
        chosen = []
        for n in range(NP):
            valid = jnp.minimum(jnp.maximum(count - n, 0), 1)
            chosen.append(FT[valid * (plist[n, 0, t] - POOL) + POOL])
        weights = jnp.concatenate([VH[slot], VL[slot]], axis=1)
        total = jnp.dot(jnp.concatenate(chosen, axis=1), weights, preferred_element_type=f32)
        total = total[:, 0:TILE] + total[:, TILE : 2 * TILE]
        target = tile_rows(MT, 49, t, 48)
        target[0:32, :] = total[0:32] + total[32:64] + total[64:96]
        target[32:48, :] = total[96:112]

    stage_power(0, 0)

    def pair_steps(step, carry):
        for inner in range(UNROLL):
            t = step * UNROLL + inner + 1
            stage_power(t, (inner + 1) % 2)
            stage_sum(t - 1, inner % 2)
        return carry

    lax.fori_loop(0, (TILES - 2) // UNROLL, pair_steps, 0)
    stage_power(TILES - 1, 1)
    stage_sum(TILES - 2, 0)
    stage_sum(TILES - 1, 1)

    own_x = [mid[c] - 0.5 for c in range(3)]
    own_line = [line[c] for c in range(3)]
    own_burgers = [burg[c] for c in range(3)]
    moments = [each_tile(MT, 49, r)[...] for r in range(32)]
    for r in range(32, 36):
        parts = [each_tile(MT, 49, r + 4 * piece)[...] for piece in range(3)]
        moments.append(parts[0] + parts[1] + parts[2])
    stress = stress_from_moments(own_x, moments)
    traction = [dot3([stress[SYM[(m, n)]] for n in range(3)], own_burgers) for m in range(3)]
    force = cross(traction, own_line)
    for c in range(3):
        for piece, value in enumerate(pieces(0.5 * force[c], 2)):
            for copy_index in range(4):
                each_tile(frow, 25, 6 * copy_index + 2 * c + piece)[...] = value
    nacc[...] = jnp.zeros_like(nacc)
    row_node = lax.broadcasted_iota(jnp.int32, (NODE_ROWS, TILE), 0) // 6

    def node_group(group, carry):
        lefts, rights = [], []
        for inner in range(NODE_GROUP):
            t = group * NODE_GROUP + inner
            rows_t = tile_rows(frow, 25, t, 24)[...]
            rows_t = jnp.concatenate([rows_t] * 9, axis=0)
            ends = nodes_in[t]
            for end in range(2):
                nodes = ends[end : end + 1, :]
                outer = row_node == lax.shift_right_logical(nodes, 7)
                lefts.append(jnp.where(outer, rows_t, 0.0).astype(bf16))
                rights.append(jnp.where(sub128 == (nodes & 127), 1.0, 0.0).astype(bf16))
        nacc[...] += lax.dot_general(
            jnp.concatenate(lefts, axis=1),
            jnp.concatenate(rights, axis=1),
            NT,
            preferred_element_type=f32,
        )
        return carry

    lax.fori_loop(0, TILES // NODE_GROUP, node_group, 0)
    for d in range(9):
        for c in range(3):
            first = 24 * d + 2 * c
            npkt[d, c] = nacc[pl.ds(first, 4, stride=6), :] + nacc[pl.ds(first + 1, 4, stride=6), :]
    node_copies = sends(2, lambda k: npkt.at[k + (k >= 4)], nrecv)
    for k in SEND_ORDER:
        node_copies[k].start()

    for copy in cell_copies:
        copy.wait()
    moments = cpkt[4]
    for q in range(8):
        moments = moments + crecv[q]
    for k in range(9):
        cout_ref[:, 35 * k : 35 * k + 35] = moments[:, 40 * k : 40 * k + 35]
    for copy in node_copies:
        copy.wait()
    nodes = npkt[4]
    for q in range(8):
        nodes = nodes + nrecv[q]
    nout_ref[...] = nodes


def hand_over(node_in, moments_in, node_out, moments_out):
    node_out[...] = node_in[...]
    moments_out[...] = moments_in[...]


def on_device(
    seg_mid, seg_line, seg_burgers, seg_cell, seg_node, ghost_list, ghost_count, pair_list, pair_count
):
    shape3 = (3, TILES, TILE)
    arguments = (
        seg_mid.reshape(shape3),
        seg_line.reshape(shape3),
        seg_burgers.reshape(shape3),
        seg_cell.reshape(TILES, TILE),
        seg_node.reshape(2, TILES, TILE).transpose(1, 0, 2),
        ghost_list.reshape(8, GHOST).T,
        ghost_count,
        pair_list.transpose(3, 0, 1, 2).reshape(NP, 1, TILES),
        pair_count,
    )
    vmem = pl.BlockSpec(memory_space=pltpu.VMEM)
    anywhere = pl.BlockSpec(memory_space=pl.ANY)
    node_force, moments = pl.pallas_call(
        kernel,
        out_shape=(
            jax.ShapeDtypeStruct((3, NODE_DEV // TILE, TILE), f32),
            jax.ShapeDtypeStruct((CELL_DEV, COMPONENTS), f32),
        ),
        in_specs=[anywhere] * 9,
        out_specs=(vmem, vmem),
        scratch_shapes=[
            pltpu.VMEM(shape3, f32),
            pltpu.VMEM(shape3, f32),
            pltpu.VMEM(shape3, f32),
            pltpu.VMEM((TILES, TILE), jnp.int32),
            pltpu.VMEM((TILES, 2, TILE), jnp.int32),
            pltpu.SMEM((GHOST, 8), jnp.int32),
            pltpu.SMEM((1, 1, 8), jnp.int32),
            pltpu.SMEM((NP, 1, TILES), jnp.int32),
            pltpu.SMEM((1, 1, TILES), jnp.int32),
            pltpu.VMEM((TILES, 16, TILE), f32),
            pltpu.VMEM((8, 9, GHOST, TILE), f32),
            pltpu.VMEM((8, 9, GHOST, TILE), f32),
            pltpu.VMEM((9, POOL - TILES, TILE), f32),
            pltpu.VMEM((POOL * 41, TILE), f32),
            pltpu.VMEM((POOL + 1, SUM_ROWS, TILE), bf16),
            pltpu.VMEM((POOL * 33, TILE), f32),
            pltpu.VMEM((POOL, TILE, TILE), bf16),
            pltpu.VMEM((TILES * 33, TILE), f32),
            pltpu.VMEM((TILES, 2 * AUG, TILE), bf16),
            pltpu.VMEM((TILES, 2 * AUG, TILE), bf16),
            pltpu.VMEM((2, NP * TILE, TILE), bf16),
            pltpu.VMEM((2, NP * TILE, TILE), bf16),
            pltpu.VMEM((TILES * 49, TILE), f32),
            pltpu.VMEM((TILES * 41, TILE), f32),
            pltpu.VMEM((TILES * 9, TILE), f32),
            pltpu.VMEM((2 * TERMS, TILE), f32),
            pltpu.VMEM((9, CELL_DEV, 384), f32),
            pltpu.VMEM((8, CELL_DEV, 384), f32),
            pltpu.VMEM((TILES * 25, TILE), f32),
            pltpu.VMEM((NODE_ROWS, TILE), f32),
            pltpu.VMEM((9, 3, 4, TILE), f32),
            pltpu.VMEM((8, 3, 4, TILE), f32),
            pltpu.SemaphoreType.DMA((3, 8)),
            pltpu.SemaphoreType.DMA((3, 8)),
            pltpu.SemaphoreType.DMA((9,)),
        ],
        compiler_params=pltpu.CompilerParams(
            collective_id=0, has_side_effects=True, vmem_limit_bytes=40 * 1024 * 1024
        ),
        name="segments",
    )(*[pltpu.with_memory_space_constraint(value, pltpu.HBM) for value in arguments])
    node_force, moments = pl.pallas_call(
        hand_over,
        out_shape=(
            jax.ShapeDtypeStruct(node_force.shape, f32),
            jax.ShapeDtypeStruct(moments.shape, f32),
        ),
        in_specs=[vmem, vmem],
        out_specs=(vmem, vmem),
        compiler_params=pltpu.CompilerParams(vmem_limit_bytes=1024 * 1024),
        name="outputs",
    )(node_force, moments)
    return node_force.reshape(1, 1, 3, NODE_DEV), moments.T


def solution(mesh):
    in_specs = (
        P("dx", "dy", None, None),
        P("dx", "dy", None, None),
        P("dx", "dy", None, None),
        P("dx", "dy", None),
        P("dx", "dy", None, None),
        P("dx", "dy", None, None),
        P("dx", "dy", None),
        P("dx", "dy", None, None),
        P("dx", "dy", None),
    )
    out_specs = (P("dx", "dy", None, None), P(None, ("dx", "dy")))
    return jax.shard_map(
        on_device, mesh=mesh, in_specs=in_specs, out_specs=out_specs, check_vma=False
    )
```

```python
import jax
import jax.numpy as jnp
from jax import lax
from jax.experimental import pallas as pl
from jax.experimental.pallas import tpu as pltpu
from jax.sharding import PartitionSpec as P

TILE = 128
TILES = 32
GHOST = 2
NP = 12
NODE_DEV = 512
CELL_DEV = 8
COMPONENTS = 315
POOL = 48
FEATURES = 40
SUM_ROWS = 112
AUG = 32
UNROLL = 30
NODE_ROWS = 216
TERMS = 368

core_radius = 0.1
shear_scale = 0.25
neighbour_offsets = ((-1, -1), (-1, 0), (-1, 1), (0, -1), (0, 1), (1, -1), (1, 0), (1, 1))
f32 = jnp.float32
bf16 = jnp.bfloat16
MESH = pl.DeviceIdType.MESH
SEND_ORDER = (0, 2, 5, 7, 1, 6, 3, 4)
NT = (((1,), (1,)), ((), ()))


def rounded(value):
    return value.astype(bf16).astype(f32)


def pieces(value, count):
    parts = []
    for _ in range(count - 1):
        part = rounded(value)
        parts.append(part)
        value = value - part
    parts.append(rounded(value))
    return parts


def each_tile(ref, pitch, index, first=0, count=TILES):
    return ref.at[pl.ds(first * pitch + index, count, stride=pitch), :]


def tile_rows(ref, pitch, t, rows):
    return ref.at[pl.ds(t * pitch, rows), :]


def exponent_table():
    exponent_rows = []
    for degree in range(5):
        for first_power in range(degree, -1, -1):
            for second in range(degree - first_power, -1, -1):
                exponent_rows.append((first_power, second, degree - first_power - second))
    return exponent_rows


def cross(u, v):
    return [
        u[1] * v[2] - u[2] * v[1],
        u[2] * v[0] - u[0] * v[2],
        u[0] * v[1] - u[1] * v[0],
    ]


def dot3(u, v):
    return u[0] * v[0] + u[1] * v[1] + u[2] * v[2]


PAIRS6 = ((0, 0), (1, 1), (2, 2), (0, 1), (0, 2), (1, 2))
SYM = {}
for _slot, (_m, _n) in enumerate(PAIRS6):
    SYM[(_m, _n)] = _slot
    SYM[(_n, _m)] = _slot


def source_features(y, line, burgers):
    g = [shear_scale * v for v in cross(burgers, line)]
    h = [[y[k] * g[n] for n in range(3)] for k in range(3)]
    q = [[y[k] * h[l][n] for n in range(3)] for (k, l) in PAIRS6]
    y2 = dot3(y, y)
    trace = h[0][0] + h[1][1] + h[2][2]
    c = []
    for m, n in PAIRS6:
        value = y2 * (h[m][n] + h[n][m]) - 3.0 * trace * (y[m] * y[n])
        if m == n:
            value = value + y2 * trace
        c.append(value)
    rows = list(g)
    for k in range(3):
        rows += h[k]
    for kl in range(6):
        rows += q[kl]
    rows += c
    return rows


def stress_from_moments(x, moment):
    c2 = core_radius**2
    G = moment[0:3]
    H = [moment[3 + 3 * k : 6 + 3 * k] for k in range(3)]
    Q = [moment[12 + 3 * kl : 15 + 3 * kl] for kl in range(6)]
    C = moment[30:36]
    x2 = dot3(x, x)
    xG = dot3(x, G)
    trH = H[0][0] + H[1][1] + H[2][2]
    Z = [Q[0][n] + Q[1][n] + Q[2][n] for n in range(3)]
    W = [Q[SYM[(0, n)]][0] + Q[SYM[(1, n)]][1] + Q[SYM[(2, n)]][2] for n in range(3)]
    xH = [x[0] * H[0][n] + x[1] * H[1][n] + x[2] * H[2][n] for n in range(3)]
    Hx = [H[n][0] * x[0] + H[n][1] * x[1] + H[n][2] * x[2] for n in range(3)]
    xQ = [
        [x[0] * Q[SYM[(0, m)]][n] + x[1] * Q[SYM[(1, m)]][n] + x[2] * Q[SYM[(2, m)]][n] for n in range(3)]
        for m in range(3)
    ]
    lead = [(x2 + c2) * G[n] - 2.0 * xH[n] + Z[n] + 3.0 * Hx[n] - 3.0 * W[n] for n in range(3)]
    both = xG - trH
    diagonal = (
        (x2 + 2.5 * c2) * both
        - 2.0 * dot3(x, xH)
        + 2.0 * dot3(x, W)
        + dot3(x, Z)
    )
    out = []
    for m, n in PAIRS6:
        value = (
            x[m] * lead[n]
            + x[n] * lead[m]
            - (x2 + c2) * (H[m][n] + H[n][m])
            + 2.0 * (xQ[m][n] + xQ[n][m])
            - 3.0 * (x[m] * x[n] * both + dot3(x, Q[SYM[(m, n)]]))
            - C[SYM[(m, n)]]
        )
        if m == n:
            value = value + diagonal
        out.append(value)
    return out


PIECE_X = (0, 0, 1, 1, 0, 2)
PIECE_Y = (0, 1, 0, 1, 2, 0)


def field_rows(x):
    one = jnp.ones_like(x[0])
    rows = []
    for c in range(3):
        part = pieces(x[c], 3)
        rows += [part[j] for j in PIECE_X]
    rows += pieces(dot3(x, x) + core_radius**2, 3)
    rows += [one, one, one]
    return rows


def source_rows(y):
    one = jnp.ones_like(y[0])
    rows = []
    for c in range(3):
        part = pieces(-2.0 * y[c], 3)
        rows += [part[j] for j in PIECE_Y]
    rows += [one, one, one]
    rows += pieces(dot3(y, y), 3)
    return rows


def kernel(
    mid_any, line_any, burg_any, cell_any, node_any, glist_any, gcount_any, plist_any, pcount_any,
    nout_ref, cout_ref,
    mid, line, burg, cells_in, nodes_in, glist, gcount, plist, pcount,
    own, pkt, ghost, far, feat, FT, yrow, YT, xrow, XL, XR, VH, VL, MT, mono, bl, cacc, cpkt,
    crecv, frow, nacc, npkt, nrecv, send_sem, recv_sem, load_sem,
):
    i = lax.axis_index("dx")
    j = lax.axis_index("dy")
    ndx = lax.axis_size("dx")
    ndy = lax.axis_size("dy")
    peers = [
        (lax.rem(i + (a + ndx), ndx), lax.rem(j + (b + ndy), ndy)) for a, b in neighbour_offsets
    ]

    barrier = pltpu.get_barrier_semaphore()
    for peer in peers:
        pl.semaphore_signal(barrier, inc=1, device_id=peer, device_id_type=MESH)

    def sends(kind, source, target):
        copies = []
        for k in range(8):
            copies.append(
                pltpu.make_async_remote_copy(
                    src_ref=source(k),
                    dst_ref=target.at[7 - k],
                    send_sem=send_sem.at[kind, k],
                    recv_sem=recv_sem.at[kind, 7 - k],
                    device_id=peers[k],
                    device_id_type=MESH,
                )
            )
        return copies

    loads = [
        pltpu.make_async_copy(source, target, load_sem.at[index])
        for index, (source, target) in enumerate(
            (
                (glist_any, glist),
                (gcount_any, gcount),
                (mid_any, mid),
                (line_any, line),
                (burg_any, burg),
                (plist_any, plist),
                (pcount_any, pcount),
                (cell_any, cells_in),
                (node_any, nodes_in),
            )
        )
    ]
    for load in loads:
        load.start()
    for load in loads:
        load.wait()

    own_flat = own.reshape(TILES * 16, TILE)
    for c in range(3):
        each_tile(own_flat, 16, c)[...] = mid[c]
        each_tile(own_flat, 16, 3 + c)[...] = line[c]
        each_tile(own_flat, 16, 6 + c)[...] = burg[c]
    for k in range(8):
        for g in range(GHOST):
            valid = jnp.minimum(jnp.maximum(gcount[0, 0, k] - g, 0), 1).astype(f32)
            pkt[k, :, g, :] = own[glist[g, k]][0:9] * valid

    ghost_copies = sends(0, lambda k: pkt.at[k], ghost)
    zero_rows = jnp.zeros((AUG, TILE), f32)

    def prepare_sources(first, count, y, line_rows, burgers, unroll):
        for index, value in enumerate(source_features(y, line_rows, burgers)):
            each_tile(feat, 41, index, first, count)[...] = value
        for index, value in enumerate(source_rows(y)):
            each_tile(yrow, 33, index, first, count)[...] = value
        zero = jnp.zeros_like(y[0])
        for index in range(36, FEATURES):
            each_tile(feat, 41, index, first, count)[...] = zero
        for index in range(24, AUG):
            each_tile(yrow, 33, index, first, count)[...] = zero

        def per_tile(t, carry):
            parts = pieces(tile_rows(feat, 41, t, FEATURES)[...], 3)
            parts = [part[0:32] for part in parts] + [part[32:36] for part in parts]
            FT[t] = jnp.concatenate(parts + [zero_rows[0:4]], axis=0).astype(bf16)
            rows_t = tile_rows(yrow, 33, t, AUG)[...]
            YT[t] = jnp.concatenate([rows_t, rows_t, zero_rows, zero_rows], axis=0).astype(bf16).T
            return carry

        lax.fori_loop(first, first + count, per_tile, 0, unroll=unroll)

    own_x = [mid[c] - 0.5 for c in range(3)]
    own_line = [line[c] for c in range(3)]
    own_burgers = [burg[c] for c in range(3)]
    prepare_sources(0, TILES, own_x, own_line, own_burgers, 8)

    field = field_rows(own_x)
    for index, value in enumerate(field):
        each_tile(xrow, 33, index)[...] = value
    for index in range(len(field), AUG):
        each_tile(xrow, 33, index)[...] = jnp.zeros((TILES, TILE), f32)

    def field_tile(t, carry):
        rows_t = tile_rows(xrow, 33, t, AUG)[...]
        XL[t] = jnp.concatenate([rows_t, zero_rows], axis=0).astype(bf16)
        XR[t] = jnp.concatenate([zero_rows, rows_t], axis=0).astype(bf16)
        return carry

    lax.fori_loop(0, TILES, field_tile, 0, unroll=8)
    FT[POOL] = jnp.zeros((SUM_ROWS, TILE), bf16)

    pl.semaphore_wait(barrier, 8)
    for k in SEND_ORDER:
        ghost_copies[k].start()

    scaled = [2.0 * (mid[c] - 0.5) for c in range(3)]
    powers = []
    for u in scaled:
        square = u * u
        powers.append([jnp.ones_like(u), u, square, square * u, square * square])
    for r, (e0, e1, e2) in enumerate(exponent_table()):
        each_tile(mono, 41, r)[...] = powers[0][e0] * powers[1][e1] * powers[2][e2]
    for r in range(35, 40):
        each_tile(mono, 41, r)[...] = jnp.zeros((TILES, TILE), f32)
    for beta in range(3):
        for gamma in range(3):
            each_tile(bl, 9, 3 * beta + gamma)[...] = burg[beta] * line[gamma]
    cacc[...] = jnp.zeros_like(cacc)
    sub128 = lax.broadcasted_iota(jnp.int32, (TILE, TILE), 0)

    def cell_group(group, carry):
        highs, lows, members = [], [], []
        for inner in range(4):
            t = group * 4 + inner
            mono_t = tile_rows(mono, 41, t, 40)[...]
            bl_t = tile_rows(bl, 9, t, 9)[...]
            block = [bl_t[k : k + 1, :] * mono_t for k in range(9)]
            block.append(jnp.zeros((8, TILE), f32))
            terms = jnp.concatenate(block, axis=0)
            high = terms.astype(bf16)
            highs.append(high)
            lows.append((terms - high.astype(f32)).astype(bf16))
            cells = cells_in[pl.ds(t, 1), :]
            members.append(jnp.where(sub128 == cells, 1.0, 0.0).astype(bf16))
        lhs = jnp.concatenate(
            [jnp.concatenate(highs, axis=1), jnp.concatenate(lows, axis=1)], axis=0
        )
        rhs = jnp.concatenate(members, axis=1)
        cacc[...] += lax.dot_general(lhs, rhs, NT, preferred_element_type=f32)
        return carry

    lax.fori_loop(0, TILES // 4, cell_group, 0)
    for block in range(3):
        rows = min(TILE, TERMS - block * TILE)
        part = cacc[block * TILE : block * TILE + rows, :] + cacc[TERMS + block * TILE : TERMS + block * TILE + rows, :]
        if rows < TILE:
            part = jnp.concatenate([part, jnp.zeros((TILE - rows, TILE), f32)], axis=0)
        turned = part.T
        for d in range(9):
            cpkt[d, :, block * TILE : (block + 1) * TILE] = turned[8 * d : 8 * d + 8, :]
    cell_copies = sends(1, lambda k: cpkt.at[k + (k >= 4)], crecv)
    for k in SEND_ORDER:
        cell_copies[k].start()

    for k in range(8):
        ghost_copies[k].wait()
    for q in range(8):
        a, b = neighbour_offsets[q]
        rows = pl.ds(GHOST * q, GHOST)
        far[0, rows, :] = ghost[q, 0] + float(a)
        far[1, rows, :] = ghost[q, 1] + float(b)
        for c in range(2, 9):
            far[c, rows, :] = ghost[q, c]
    prepare_sources(
        TILES,
        POOL - TILES,
        [far[c] - 0.5 for c in range(3)],
        [far[c] for c in range(3, 6)],
        [far[c] for c in range(6, 9)],
        16,
    )

    first_half = lax.broadcasted_iota(jnp.int32, (TILE, TILE), 1) < AUG

    def stage_power(t, slot):
        rhs = jnp.concatenate([XL[t], XR[t]], axis=1)
        for pair in range(NP // 2):
            lhs = jnp.where(first_half, YT[plist[2 * pair, 0, t]], YT[plist[2 * pair + 1, 0, t]])
            both = jnp.dot(lhs[:, 0 : 2 * AUG], rhs, preferred_element_type=f32)
            for side in range(2):
                inverse = lax.rsqrt(both[:, side * TILE : (side + 1) * TILE])
                square = inverse * inverse
                value = square * square * inverse
                high = value.astype(bf16)
                first = (2 * pair + side) * TILE
                VH[slot, first : first + TILE, :] = high
                VL[slot, first : first + TILE, :] = (value - high.astype(f32)).astype(bf16)

    def stage_sum(t, slot):
        count = pcount[0, 0, t]
        chosen = []
        for n in range(NP):
            valid = jnp.minimum(jnp.maximum(count - n, 0), 1)
            chosen.append(FT[valid * (plist[n, 0, t] - POOL) + POOL])
        weights = jnp.concatenate([VH[slot], VL[slot]], axis=1)
        total = jnp.dot(jnp.concatenate(chosen, axis=1), weights, preferred_element_type=f32)
        total = total[:, 0:TILE] + total[:, TILE : 2 * TILE]
        target = tile_rows(MT, 49, t, 48)
        target[0:32, :] = total[0:32] + total[32:64] + total[64:96]
        target[32:48, :] = total[96:112]

    stage_power(0, 0)

    def pair_steps(step, carry):
        for inner in range(UNROLL):
            t = step * UNROLL + inner + 1
            stage_power(t, (inner + 1) % 2)
            stage_sum(t - 1, inner % 2)
        return carry

    lax.fori_loop(0, (TILES - 2) // UNROLL, pair_steps, 0)
    row_node = lax.broadcasted_iota(jnp.int32, (NODE_ROWS, TILE), 0) // 6

    def scatter(first, count):
        rows = slice(first, first + count)
        x = [mid[c, rows] - 0.5 for c in range(3)]
        moments = [each_tile(MT, 49, r, first, count)[...] for r in range(32)]
        for r in range(32, 36):
            parts = [each_tile(MT, 49, r + 4 * piece, first, count)[...] for piece in range(3)]
            moments.append(parts[0] + parts[1] + parts[2])
        stress = stress_from_moments(x, moments)
        burgers = [burg[c, rows] for c in range(3)]
        traction = [dot3([stress[SYM[(m, n)]] for n in range(3)], burgers) for m in range(3)]
        force = cross(traction, [line[c, rows] for c in range(3)])
        for c in range(3):
            for piece, value in enumerate(pieces(0.5 * force[c], 2)):
                for copy_index in range(4):
                    each_tile(frow, 25, 6 * copy_index + 2 * c + piece, first, count)[...] = value
        lefts, rights = [], []
        for t in range(first, first + count):
            rows_t = tile_rows(frow, 25, t, 24)[...]
            rows_t = jnp.concatenate([rows_t] * 9, axis=0)
            ends = nodes_in[t]
            for end in range(2):
                nodes = ends[end : end + 1, :]
                outer = row_node == lax.shift_right_logical(nodes, 7)
                lefts.append(jnp.where(outer, rows_t, 0.0).astype(bf16))
                rights.append(jnp.where(sub128 == (nodes & 127), 1.0, 0.0).astype(bf16))
        return lax.dot_general(
            jnp.concatenate(lefts, axis=1),
            jnp.concatenate(rights, axis=1),
            NT,
            preferred_element_type=f32,
        )

    stage_power(TILES - 1, 1)
    early = scatter(0, TILES // 2)
    stage_sum(TILES - 2, 0)
    stage_sum(TILES - 1, 1)

    nacc[...] = early + scatter(TILES // 2, TILES // 2)
    for d in range(9):
        for c in range(3):
            first = 24 * d + 2 * c
            npkt[d, c] = nacc[pl.ds(first, 4, stride=6), :] + nacc[pl.ds(first + 1, 4, stride=6), :]
    node_copies = sends(2, lambda k: npkt.at[k + (k >= 4)], nrecv)
    for k in SEND_ORDER:
        node_copies[k].start()

    for copy in cell_copies:
        copy.wait()
    moments = cpkt[4]
    for q in range(8):
        moments = moments + crecv[q]
    for k in range(9):
        cout_ref[:, 35 * k : 35 * k + 35] = moments[:, 40 * k : 40 * k + 35]
    for copy in node_copies:
        copy.wait()
    nodes = npkt[4]
    for q in range(8):
        nodes = nodes + nrecv[q]
    nout_ref[...] = nodes


def hand_over(node_in, moments_in, node_out, moments_out):
    node_out[...] = node_in[...]
    moments_out[...] = moments_in[...]


def on_device(
    seg_mid, seg_line, seg_burgers, seg_cell, seg_node, ghost_list, ghost_count, pair_list, pair_count
):
    shape3 = (3, TILES, TILE)
    arguments = (
        seg_mid.reshape(shape3),
        seg_line.reshape(shape3),
        seg_burgers.reshape(shape3),
        seg_cell.reshape(TILES, TILE),
        seg_node.reshape(2, TILES, TILE).transpose(1, 0, 2),
        ghost_list.reshape(8, GHOST).T,
        ghost_count,
        pair_list.transpose(3, 0, 1, 2).reshape(NP, 1, TILES),
        pair_count,
    )
    vmem = pl.BlockSpec(memory_space=pltpu.VMEM)
    anywhere = pl.BlockSpec(memory_space=pl.ANY)
    node_force, moments = pl.pallas_call(
        kernel,
        out_shape=(
            jax.ShapeDtypeStruct((3, NODE_DEV // TILE, TILE), f32),
            jax.ShapeDtypeStruct((CELL_DEV, COMPONENTS), f32),
        ),
        in_specs=[anywhere] * 9,
        out_specs=(vmem, vmem),
        scratch_shapes=[
            pltpu.VMEM(shape3, f32),
            pltpu.VMEM(shape3, f32),
            pltpu.VMEM(shape3, f32),
            pltpu.VMEM((TILES, TILE), jnp.int32),
            pltpu.VMEM((TILES, 2, TILE), jnp.int32),
            pltpu.SMEM((GHOST, 8), jnp.int32),
            pltpu.SMEM((1, 1, 8), jnp.int32),
            pltpu.SMEM((NP, 1, TILES), jnp.int32),
            pltpu.SMEM((1, 1, TILES), jnp.int32),
            pltpu.VMEM((TILES, 16, TILE), f32),
            pltpu.VMEM((8, 9, GHOST, TILE), f32),
            pltpu.VMEM((8, 9, GHOST, TILE), f32),
            pltpu.VMEM((9, POOL - TILES, TILE), f32),
            pltpu.VMEM((POOL * 41, TILE), f32),
            pltpu.VMEM((POOL + 1, SUM_ROWS, TILE), bf16),
            pltpu.VMEM((POOL * 33, TILE), f32),
            pltpu.VMEM((POOL, TILE, TILE), bf16),
            pltpu.VMEM((TILES * 33, TILE), f32),
            pltpu.VMEM((TILES, 2 * AUG, TILE), bf16),
            pltpu.VMEM((TILES, 2 * AUG, TILE), bf16),
            pltpu.VMEM((2, NP * TILE, TILE), bf16),
            pltpu.VMEM((2, NP * TILE, TILE), bf16),
            pltpu.VMEM((TILES * 49, TILE), f32),
            pltpu.VMEM((TILES * 41, TILE), f32),
            pltpu.VMEM((TILES * 9, TILE), f32),
            pltpu.VMEM((2 * TERMS, TILE), f32),
            pltpu.VMEM((9, CELL_DEV, 384), f32),
            pltpu.VMEM((8, CELL_DEV, 384), f32),
            pltpu.VMEM((TILES * 25, TILE), f32),
            pltpu.VMEM((NODE_ROWS, TILE), f32),
            pltpu.VMEM((9, 3, 4, TILE), f32),
            pltpu.VMEM((8, 3, 4, TILE), f32),
            pltpu.SemaphoreType.DMA((3, 8)),
            pltpu.SemaphoreType.DMA((3, 8)),
            pltpu.SemaphoreType.DMA((9,)),
        ],
        compiler_params=pltpu.CompilerParams(
            collective_id=0, has_side_effects=True, vmem_limit_bytes=40 * 1024 * 1024
        ),
        name="segments",
    )(*[pltpu.with_memory_space_constraint(value, pltpu.HBM) for value in arguments])
    node_force, moments = pl.pallas_call(
        hand_over,
        out_shape=(
            jax.ShapeDtypeStruct(node_force.shape, f32),
            jax.ShapeDtypeStruct(moments.shape, f32),
        ),
        in_specs=[vmem, vmem],
        out_specs=(vmem, vmem),
        compiler_params=pltpu.CompilerParams(vmem_limit_bytes=1024 * 1024),
        name="outputs",
    )(node_force, moments)
    return node_force.reshape(1, 1, 3, NODE_DEV), moments.T


def solution(mesh):
    in_specs = (
        P("dx", "dy", None, None),
        P("dx", "dy", None, None),
        P("dx", "dy", None, None),
        P("dx", "dy", None),
        P("dx", "dy", None, None),
        P("dx", "dy", None, None),
        P("dx", "dy", None),
        P("dx", "dy", None, None),
        P("dx", "dy", None),
    )
    out_specs = (P("dx", "dy", None, None), P(None, ("dx", "dy")))
    return jax.shard_map(
        on_device, mesh=mesh, in_specs=in_specs, out_specs=out_specs, check_vma=False
    )
```
